32 devices in a mesh: grp: 2 (over core), dev: 16 (over z, y, x).
Axes of the slice: x: 2, y: 2, z: 4, core: 2. Of those that a mesh axis runs over, the one named last changes fastest.
Arguments:
- accum: float32 [4096, 24, 128], P(('grp', 'dev')), may hold values from -48 to 48
- step_count: int32 [24], replicated, may hold values from 1 to 12
- stretch_slot: int32 [4096], replicated, may hold values from 0 to 4095, as said below
- span_length: int32 [32], replicated, may hold values from 1 to 256, 4096 in all
- wet_mask: int32 [8192], P(('grp', 'dev')), may hold values 0 or 1
Outputs:
- ocean_flux: float32 [8192, 24, 128], P(('grp', 'dev'))
The draws below stay inside these ranges and needn't reach their ends.
Inputs may be any that keep to these rules, and one draw needn't show every extreme that they name: `stretch_slot`: A permutation of the slots; any 32 consecutive row blocks lie on 32 different atmosphere devices (slot // 128). `span_length`: sums to 4096; some ocean device owns exactly 256 blocks. `wet_mask`: entries of slots beyond an ocean device's span are ignored.
All inputs are finite; a program needn't handle non-finite values.
Results may differ from the reference program's by a relative error of at most 0.000071.
Values sent between devices are 32-bit elements; how exact they have to be, the bound alone decides.
A program may use at most 64 MiB of HBM per device.

```python
import math
import jax
import jax.numpy as jnp
import numpy as np

FIELDS = 24
CELLS = 128
BLOCKS_DEV = 128
DEVICE_COUNT = 32
ALL_BLOCKS = 4096
CAPACITY = 256


def draw_stretch_slot(key, part):
    devices = ALL_BLOCKS // BLOCKS_DEV
    first_key = jax.random.fold_in(key, 11)
    second_key = jax.random.fold_in(key, 12)
    dealing = jax.random.permutation(first_key, devices).astype(jnp.int32)
    rotation = jax.random.randint(second_key, (devices,), 0, BLOCKS_DEV).astype(jnp.int32)
    global_ids = jnp.arange(ALL_BLOCKS, dtype=jnp.int32)
    holder = dealing[global_ids % devices]
    local_slot = (global_ids // devices + rotation[holder]) % BLOCKS_DEV
    return (holder * BLOCKS_DEV + local_slot).astype(jnp.int32)


def set_ends(drawn, own_key, least, largest):
    extent = drawn.shape
    index_at = [jax.random.randint(jax.random.fold_in(own_key, axis), (), 0, extent[axis]) for axis in range(len(extent))]
    drawn = drawn.at[tuple(index_at)].set(least)
    longest = extent.index(max(extent))
    index_at[longest] = (index_at[longest] + 1) % extent[longest]
    return drawn.at[tuple(index_at)].set(largest)


def level_of(rng, shape, cuts, low, high):
    def one(axis_at, shards_of):
        draws = jax.random.uniform(jax.random.fold_in(jax.random.fold_in(rng, 6), axis_at), (shards_of,), jnp.float32, low / len(cuts), high / len(cuts))
        return jnp.repeat(jnp.exp(draws), shape[axis_at] // shards_of).reshape((-1,) + (1,) * (len(shape) - axis_at - 1))

    factor_of = one(*cuts[0])
    for cut in cuts[1:]:
        factor_of = factor_of * one(*cut)
    return factor_of


def profile(amount, total, limit, lean):
    weights = [(1 << 20) // math.isqrt(rank ** lean) + 1 for rank in range(2, amount + 1)]
    surplus, given = total - limit - (amount - 1), [1] * (amount - 1)
    while surplus > 0:
        free = [i for i in range(amount - 1) if given[i] < limit]
        mass, remaining = sum([weights[i] for i in free]), surplus
        for i in free:
            more = min(limit - given[i], max(1, remaining * weights[i] // mass), surplus)
            given[i] = given[i] + more
            surplus = surplus - more
    return np.array([limit] + given)


def ragged(rng, number_of, total, reach, slope):
    if number_of == 2:
        one = jax.random.randint(rng, (), max(1, total - reach), min(reach, total - 1) + 1)
        return jnp.stack([one, total - one])
    tallies = jnp.asarray(profile(number_of, total, reach, slope), jnp.int32)
    twos = (number_of - 1) // 2
    source_of, receiver = tallies[1:1 + 2 * twos:2], tallies[2:2 + 2 * twos:2]
    slack = jnp.minimum(source_of - 1, reach - receiver)
    moved = jax.random.randint(jax.random.fold_in(rng, 1), (twos,), 0, 1 << 20) % (slack + 1)
    tallies = tallies.at[1:1 + 2 * twos:2].set(source_of - moved).at[2:2 + 2 * twos:2].set(receiver + moved)
    return tallies[jax.random.permutation(jax.random.fold_in(rng, 2), number_of)]


def noise(rng, shape, scale, most, pieces=(), kind=jnp.bfloat16):
    values = jax.random.normal(rng, shape, jnp.float32) * scale
    if len(pieces) > 0:
        values = level_of(rng, shape, pieces, -0.22, 0.18) * values
    return jnp.clip(values, min=-most, max=most).astype(kind)


def setup_inputs(seed: int = 0) -> dict:
    keys = jax.random.split(jax.random.key(seed), 6)
    accum = noise(keys[0], (ALL_BLOCKS, FIELDS, CELLS), 8.0, 48.0, ((0, 32),), jnp.float32)
    step_count = set_ends(jax.random.randint(keys[1], (FIELDS,), 1, 13), jax.random.fold_in(keys[1], 1), 1, 12).astype(jnp.int32)
    stretch_slot = draw_stretch_slot(jax.random.fold_in(keys[5], 71), 0)
    span_length = ragged(keys[3], DEVICE_COUNT, ALL_BLOCKS, CAPACITY, 2).astype(jnp.int32)
    wet_mask = set_ends((jax.random.randint(keys[4], (DEVICE_COUNT * CAPACITY,), 0, 4) < 3).astype(jnp.int32), jax.random.fold_in(keys[4], 1), 0, 1)
    return dict(accum=accum, step_count=step_count, stretch_slot=stretch_slot, span_length=span_length, wet_mask=wet_mask)


def reference(accum, step_count, stretch_slot, span_length, wet_mask):
    span_end = jnp.cumsum(span_length).astype(jnp.int32)
    span_start = (span_end - span_length).astype(jnp.int32)
    global_ids = jnp.arange(ALL_BLOCKS, dtype=jnp.int32)
    owner = jnp.sum((span_end[None, :] <= global_ids[:, None]).astype(jnp.int32), axis=1).astype(jnp.int32)
    position = (owner * CAPACITY + global_ids - span_start[owner]).astype(jnp.int32)
    wet = (wet_mask[position] == 1).astype(jnp.float32)
    counts = step_count.astype(jnp.float32)
    masked = (accum[stretch_slot] / counts[None, :, None]) * wet[:, None, None]
    flat = jnp.transpose(masked, (1, 0, 2)).reshape(FIELDS, ALL_BLOCKS * CELLS)
    zero_col = jnp.zeros((FIELDS, 1), jnp.float32)
    before = jnp.concatenate([zero_col, flat[:, :-1]], axis=1)
    after_cells = jnp.concatenate([flat[:, 1:], zero_col], axis=1)
    smoothed = 0.25 * before + 0.5 * flat + 0.25 * after_cells
    smoothed = jnp.transpose(smoothed.reshape(FIELDS, ALL_BLOCKS, CELLS), (1, 0, 2)) * wet[:, None, None]
    result = jnp.zeros((DEVICE_COUNT * CAPACITY, FIELDS, CELLS), jnp.float32)
    return result.at[position].set(smoothed)
```

```python
import functools
import jax
import jax.numpy as jnp
from jax import lax
from jax.experimental import pallas as pl
from jax.experimental.pallas import tpu as pltpu
from jax.sharding import PartitionSpec as P

MESH = pl.DeviceIdType.MESH
SPARES = ((4, 24), (6, 24), (8, 24), (10, 24), (12, 24), (14, 24), (16, 24), (20, 24), (12, 32), (20, 32), (32, 32))


def exchange_kernel(
    sizes, stretch, spans, wet, accum, received, halo,
    starts, packed, landed, edge_out, edge_in, send_sem, recv_sem, out_sem, edge_send, edge_recv, edge_copy,
):
    groups, chips, layers, pair_most, blocks_dev, all_blocks = sizes
    devices = groups * chips
    plane = chips // layers
    grp = lax.axis_index("grp")
    dev = lax.axis_index("dev")
    me = grp * chips + dev
    layer, place = dev // plane, dev % plane

    def at(index):
        return (index // chips, index % chips)

    barrier = pltpu.get_barrier_semaphore()

    @pl.loop(1, devices)
    def _(step):
        pl.semaphore_signal(barrier, inc=1, device_id=at((me + step) % devices), device_id_type=MESH)

    def prefix(owner, total):
        starts[owner] = total
        return total + spans[owner]

    lax.fori_loop(0, devices, prefix, jnp.int32(0))

    def find(block, found):
        return jnp.where(stretch[block] // blocks_dev == me, block, found)

    phase = lax.fori_loop(0, devices, find, jnp.int32(0), unroll=8)

    def partner(turn, rest):
        there = ((layer + turn) % layers) * plane + (place + rest % plane) % plane
        return ((grp + rest // plane) % groups) * chips + there

    def pack(owner, target, base):
        start = starts[owner]
        first = start + lax.rem(phase - start + all_blocks * devices, devices)
        for rank in range(pair_most):
            block = jnp.minimum(first + rank * devices, all_blocks - 1)
            slot = lax.rem(stretch[block], blocks_dev)
            target[base + rank] = accum[slot]

    def send_copy(other):
        return pltpu.make_async_remote_copy(
            src_ref=packed.at[pl.ds(other * pair_most, pair_most)],
            dst_ref=landed.at[pl.ds(me * pair_most, pair_most)],
            send_sem=send_sem.at[other],
            recv_sem=recv_sem.at[me],
            device_id=at(other),
            device_id_type=MESH,
        )

    def out_copy(other):
        return pltpu.make_async_copy(
            landed.at[pl.ds(other * pair_most, pair_most)],
            received.at[pl.ds(other * pair_most, pair_most)],
            out_sem.at[other],
        )

    turns = [layers // 2] + [t for t in range(1, layers) if t != layers // 2]
    if layers > 1:
        turns = turns + [0]
    else:
        turns = [0]
    rests = groups * plane
    for number, turn in enumerate(turns):
        low = 1 if turn == 0 else 0

        @pl.loop(low, rests)
        def _(rest):
            other = partner(turn, rest)
            pack(other, packed, other * pair_most)

        if number == 0:
            pl.semaphore_wait(barrier, devices - 1)

        @pl.loop(low, rests)
        def _(rest):
            send_copy(partner(turn, rest)).start()

    pack(me, landed, me * pair_most)

    for turn in reversed(turns):
        low = 1 if turn == 0 else 0

        @pl.loop(low, rests)
        def _(rest):
            other = partner(turn, rest)
            pltpu.make_async_remote_copy(
                src_ref=packed.at[pl.ds(other * pair_most, pair_most)],
                dst_ref=landed.at[pl.ds(other * pair_most, pair_most)],
                send_sem=send_sem.at[other],
                recv_sem=recv_sem.at[other],
                device_id=at(other),
                device_id_type=MESH,
            ).wait_recv()
            out_copy(other).start()

    out_copy(me).start()

    start = starts[me]
    length = spans[me]
    first_from = stretch[start] // blocks_dev
    last = jnp.maximum(length - 1, 0)
    last_from = stretch[start + last] // blocks_dev
    edge_out[0] = landed[last_from * pair_most + last // devices] * (
        wet[last] == 1
    ).astype(jnp.float32)
    edge_out[1] = landed[first_from * pair_most] * (wet[0] == 1).astype(jnp.float32)
    copies = []
    for side, shift in ((0, 1), (1, devices - 1)):
        copies.append(
            pltpu.make_async_remote_copy(
                src_ref=edge_out.at[side],
                dst_ref=edge_in.at[side],
                send_sem=edge_send.at[side],
                recv_sem=edge_recv.at[side],
                device_id=at((me + shift) % devices),
                device_id_type=MESH,
            )
        )
    for copy in copies:
        copy.start()

    @pl.loop(1, devices)
    def _(step):
        send_copy((me + step) % devices).wait_send()

    @pl.loop(0, devices)
    def _(other):
        out_copy(other).wait()

    for copy in copies:
        copy.wait()
    final = pltpu.make_async_copy(edge_in, halo, edge_copy)
    final.start()
    final.wait()


def stream_kernel(
    sizes, spare, early, stretch, spans, wet, accum_at, received, halo,
    starts, accum, to_mate, to_spare, to_near, to_far, lists, merged, forward, edge_all, edge_near,
    load_sem, mate_send, mate_recv, spare_send, spare_recv, pass_send, main_send, main_recv,
    near_send, near_recv, edge_send, edge_recv,
):
    groups, chips, layers, pair_most, blocks_dev, all_blocks = sizes
    devices = groups * chips
    plane = chips // layers
    rests = groups * plane
    main = rests * pair_most // 2
    room = main + spare
    _, fields, cells = accum.shape
    shift = devices.bit_length() - 1
    grp = lax.axis_index("grp")
    dev = lax.axis_index("dev")
    me = grp * chips + dev
    layer, place = dev // plane, dev % plane
    low = layer < 2
    inner = (layer == 1) | (layer == 2)
    across = (
        layer, layer + 1 - 2 * (layer % 2), jnp.where(low, 2, 1), jnp.where(low, 3, 0)
    )
    my_spot = grp * plane + place

    def at(index):
        return (index // chips, index % chips)

    def column(there):
        return grp * chips + there * plane + place

    def mate(spot):
        return (spot // plane) * chips + layer * plane + spot % plane

    load = pltpu.make_async_copy(accum_at, accum, load_sem)
    load.start()
    barrier = pltpu.get_barrier_semaphore()
    for turn in (1, 2, 3):
        pl.semaphore_signal(
            barrier, inc=1, device_id=at(column((layer + turn) % layers)), device_id_type=MESH
        )

    @pl.loop(1, rests)
    def _(step):
        pl.semaphore_signal(
            barrier, inc=1, device_id=at(mate((my_spot + step) % rests)), device_id_type=MESH
        )

    def prefix(owner, total):
        starts[owner] = total
        return total + spans[owner]

    starts[devices] = lax.fori_loop(0, devices, prefix, jnp.int32(0), unroll=8)

    def find(block, found):
        holder = lax.div(stretch[block], blocks_dev)
        return tuple(
            jnp.where(holder == column(across[turn]), block, found[turn]) for turn in range(4)
        )

    phases = lax.fori_loop(0, devices, find, (jnp.int32(0),) * 4, unroll=8)

    def rank_of(phase, owner):
        return lax.shift_right_arithmetic(starts[owner] + (devices - 1) - phase, jnp.int32(shift))

    def layer_list(phase, there):
        marks = []
        for part in range(2):
            first = part * chips + there * plane
            begin = rank_of(phase, first)
            marks.append((begin, rank_of(phase, first + plane) - begin))
        (begin_low, amount), (begin_high, more) = marks
        return amount, begin_low, begin_high - amount, amount + more

    def slot_of(rank, phase):
        block = jnp.minimum(phase + rank * devices, all_blocks - 1)
        return lax.rem(stretch[block], blocks_dev)

    mine = phases[0]
    lists_to = [layer_list(mine, across[turn]) for turn in range(4)]

    def block_at(listed, spot):
        amount, begin_low, begin_high, _ = listed
        return accum[slot_of(spot + jnp.where(spot < amount, begin_low, begin_high), mine)]

    def fill(target, begin, end, listed):
        def one(spot, carry):
            target[spot] = block_at(listed, spot)
            return carry

        lax.fori_loop(begin, end, one, jnp.int32(0), unroll=4)

    far_list = jnp.where(inner, 1, 2)

    def pick(turn, values):
        if turn == "first":
            return jnp.where(inner, values[2], values[3])
        if turn == "second":
            return jnp.where(inner, values[3], values[2])
        return values[turn]

    def order(turn):
        return {"first": 2, "second": 3}.get(turn, turn)

    def mate_copy(step):
        begin, end = ((0, early), (early, room + 1))[step]
        return pltpu.make_async_remote_copy(
            src_ref=to_mate.at[pl.ds(begin, end - begin)],
            dst_ref=lists.at[0, pl.ds(begin, end - begin)],
            send_sem=mate_send.at[step],
            recv_sem=mate_recv.at[step],
            device_id=at(column(across[1])),
            device_id_type=MESH,
        )

    def spare_copy(where):
        return pltpu.make_async_remote_copy(
            src_ref=to_spare,
            dst_ref=lists.at[where, pl.ds(main, spare + 1)],
            send_sem=spare_send,
            recv_sem=spare_recv.at[where],
            device_id=at(column(across[2])),
            device_id_type=MESH,
        )

    def pass_copy(where):
        return pltpu.make_async_remote_copy(
            src_ref=lists.at[where, pl.ds(main, spare + 1)],
            dst_ref=lists.at[where, pl.ds(main, spare + 1)],
            send_sem=pass_send.at[where],
            recv_sem=spare_recv.at[where],
            device_id=at(column(across[1])),
            device_id_type=MESH,
        )

    cuts = [(0, early), (early, main)] if early < main else [(0, main)]

    def main_copy(outer, step, where):
        begin, end = cuts[step]
        return pltpu.make_async_remote_copy(
            src_ref=(to_far if outer else to_near).at[pl.ds(begin, end - begin)],
            dst_ref=lists.at[where, pl.ds(begin, end - begin)],
            send_sem=main_send.at[outer, step],
            recv_sem=main_recv.at[where, step],
            device_id=at(column(across[3 if outer else 2])),
            device_id_type=MESH,
        )

    def near_copy(turn, spot, sender):
        return pltpu.make_async_remote_copy(
            src_ref=forward.at[pl.ds((order(turn) * rests + spot) * pair_most, pair_most)],
            dst_ref=received.at[pl.ds(sender * pair_most, pair_most)],
            send_sem=near_send.at[order(turn) * rests + spot],
            recv_sem=near_recv.at[sender],
            device_id=at(mate(spot)),
            device_id_type=MESH,
        )

    def edge_copy(spot, sender):
        return pltpu.make_async_remote_copy(
            src_ref=edge_all,
            dst_ref=edge_near.at[sender],
            send_sem=edge_send.at[spot],
            recv_sem=edge_recv.at[sender],
            device_id=at(mate(spot)),
            device_id_type=MESH,
        )

    def hand_on(turn, begin, end, limit):
        listed = pick(turn, (0, 0, 1, 2))
        phase = pick(turn, phases)
        sender = column(pick(turn, across))
        if turn != 0:
            amount, begin_low, begin_high, _ = layer_list(phase, layer)
            jump = jnp.int32(0)
            if turn != 1:
                other = layer_list(phase, across[1])[3]
                jump = jnp.where(inner, jnp.maximum(other - main, 0), 0)

        def put(spot, target, base):
            owner = mate(spot)
            first = rank_of(phase, owner)
            if turn != 0:
                first = first - jnp.where(spot < plane, begin_low, begin_high)
            for step in range(pair_most):
                if turn == 0:
                    target[base + step] = accum[slot_of(first + step, phase)]
                else:
                    row = first + step
                    if turn != 1:
                        row = row + jnp.where(row < main, 0, jump)
                    target[base + step] = merged[listed, jnp.clip(row, 0, limit - 1)]

        @pl.loop(begin, end)
        def _(spot):
            @pl.when(spot != my_spot)
            def _():
                put(spot, forward, (order(turn) * rests + spot) * pair_most)

            @pl.when(spot == my_spot)
            def _():
                put(spot, received, sender * pair_most)

        @pl.loop(begin, end)
        def _(spot):
            @pl.when(spot != my_spot)
            def _():
                near_copy(turn, spot, sender).start()

    load.wait()
    fill(to_mate, 0, early, lists_to[1])

    @pl.when(inner)
    def _():
        fill(to_near, 0, cuts[0][1], lists_to[2])

    pl.semaphore_wait(barrier, layers - 1 + rests - 1)
    mate_copy(0).start()

    @pl.when(inner)
    def _():
        main_copy(0, 0, far_list).start()

    hand_on(0, 0, rests, None)

    lane = lax.broadcasted_iota(jnp.int32, (fields, cells), 1)
    ending = jnp.maximum(spans[me] - 1, 0)
    edges = jnp.where(
        lane == 2 * (devices + me),
        jnp.where(wet[0] == 1, 1.0, 0.0),
        jnp.where(
            lane == 2 * (devices + me) + 1, jnp.where(wet[ending] == 1, 1.0, 0.0), 0.0
        ),
    )

    def collect(owner, edges):
        for back, turned in ((1, 2 * owner), (0, 2 * owner - 1)):
            held = stretch[jnp.clip(starts[owner] - back, 0, all_blocks - 1)]
            rolled = pltpu.roll(accum[lax.rem(held, blocks_dev)], (turned + back) % cells, 1)
            wanted = jnp.where(lax.div(held, blocks_dev) == me, turned, -1)
            edges = jnp.where(lane == wanted, rolled, edges)
        return edges

    edges = lax.fori_loop(1, devices, collect, edges, unroll=2)
    to_mate[room] = edges
    to_spare[spare] = edges
    over = jnp.maximum(lists_to[3][3] - main, 0)

    def fill_spare(spot, carry):
        rank = []
        for listed, back in ((lists_to[3], 0), (lists_to[2], over)):
            amount, begin_low, begin_high, _ = listed
            there = main + spot - back
            rank.append(there + jnp.where(there < amount, begin_low, begin_high))
        to_spare[spot] = accum[slot_of(jnp.where(spot < over, rank[0], rank[1]), mine)]
        return carry

    lax.fori_loop(0, spare, fill_spare, jnp.int32(0), unroll=2)
    fill(to_mate, early, room, lists_to[1])
    spare_copy(far_list).start()
    mate_copy(1).start()
    last = len(cuts) - 1

    @pl.when(inner)
    def _():
        fill(to_far, 0, main, lists_to[3])
        for step in range(last + 1):
            main_copy(1, step, far_list).start()
        if last:
            fill(to_near, cuts[1][0], main, lists_to[2])
            main_copy(0, 1, far_list).start()

    @pl.when(jnp.logical_not(inner))
    def _():
        for step in range(last + 1):
            fill(to_far, *cuts[step], lists_to[3])
            fill(to_near, *cuts[step], lists_to[2])
            main_copy(1, step, far_list).start()
            main_copy(0, step, far_list).start()

    near_group = (0, plane, early) if last else (0, rests, room)
    far_group = (plane, rests, room)

    def merge(where, begin, end):
        part = pl.ds(begin, end - begin)
        merged[where, part] = lists[where, part]

    def arrive(where, step):
        main_copy(0, step, where).wait_recv()
        merge(where, *cuts[step])

    def spared(where):
        spare_copy(where).wait_recv()
        merge(where, main, room)

    @pl.when(inner)
    def _():
        spared(1)
        pass_copy(1).start()
        spared(2)
        pass_copy(2).start()

    mate_copy(0).wait_recv()
    merge(0, 0, early)
    hand_on(1, 0, plane, early)

    @pl.when(inner)
    def _():
        arrive(1, 0)
        hand_on(2, *near_group)

    mate_copy(1).wait_recv()
    merge(0, early, room)
    hand_on(1, plane, rests, room)

    @pl.when(jnp.logical_not(inner))
    def _():
        spared(2)

    arrive(2, 0)
    hand_on(3, *near_group)
    if last:
        arrive(2, 1)
        hand_on(3, *far_group)

    @pl.when(jnp.logical_not(inner))
    def _():
        spared(1)

    total = edges
    for where in range(3):
        total = total + lists[where, room]
    edge_all[...] = total

    @pl.loop(0, rests)
    def _(spot):
        @pl.when(spot != my_spot)
        def _():
            edge_copy(spot, my_spot).start()

    @pl.when(jnp.logical_not(inner))
    def _():
        arrive(1, 0)
        hand_on(2, *near_group)

    if last:
        arrive(1, 1)
        hand_on(2, *far_group)

    @pl.when(inner)
    def _():
        for where in (1, 2):
            pass_copy(where).wait_send()

    for step in range(2):
        mate_copy(step).wait_send()
    spare_copy(far_list).wait_send()
    for outer in range(2):
        for step in range(last + 1):
            main_copy(outer, step, far_list).wait_send()

    edge_near[my_spot] = total

    @pl.loop(0, rests)
    def _(spot):
        @pl.when(spot != my_spot)
        def _():
            edge_copy(spot, spot).wait()

    total = edge_near[0]
    for spot in range(1, rests):
        total = total + edge_near[spot]
    spread = cells * devices

    def cell(to, lane_from):
        return pltpu.roll(total, lax.rem(to - lane_from + spread, cells), 1)

    wet_left, wet_right = 2 * (devices + me) - 1, 2 * (devices + me) + 2
    halo[0] = cell(cells - 1, 2 * me) * cell(cells - 1, wet_left)
    halo[1] = cell(0, 2 * me + 1) * cell(0, wet_right)

    @pl.loop(0, rests)
    def _(spot):
        @pl.when(spot != my_spot)
        def _():
            for turn in range(4):
                sender = (spot // plane) * chips + across[turn] * plane + spot % plane
                near_copy(turn, spot, sender).wait()


def filter_kernel(sizes, stretch, spans, wet, counts, received, halo, out, rows, done, sem):
    groups, chips, pair_most, blocks_dev, all_blocks = sizes
    devices = groups * chips
    me = lax.axis_index("grp") * chips + lax.axis_index("dev")
    length = spans[me]
    capacity = wet.shape[0]
    _, fields, cells = halo.shape
    start = lax.fori_loop(
        0, devices, lambda o, s: s + jnp.where(o < me, spans[o], 0), jnp.int32(0), unroll=8
    )

    def fill(spot, carry):
        block = jnp.minimum(start + spot, all_blocks - 1)
        rows[spot] = lax.div(stretch[block], blocks_dev) * pair_most
        return carry

    lax.fori_loop(0, devices, fill, jnp.int32(0), unroll=8)
    rows[devices] = rows[0] + 1
    field = lax.broadcasted_iota(jnp.int32, (fields, cells), 0)
    held = jnp.ones((fields, cells), jnp.int32)
    for index in range(fields):
        held = jnp.where(field == index, counts[index], held)
    scale = 0.25 / held.astype(jnp.float32)
    lane = lax.broadcasted_iota(jnp.int32, (fields, cells), 1)
    at_first, at_last = lane == 0, lane == cells - 1
    left = halo[0] * jnp.where(me > 0, 1.0, 0.0)
    right = halo[1] * jnp.where(me < devices - 1, 1.0, 0.0)

    def wet_of(slot):
        return jnp.where(slot < length, wet[slot], 0).astype(jnp.float32)

    def out_copy(rank):
        part = pl.ds(rank * devices, devices)
        return pltpu.make_async_copy(done.at[part], out.at[part], sem.at[rank])

    def one_rank(rank, carry):
        def one(spot, carry):
            before, here, mask = carry
            slot = rank * devices + spot
            later = jnp.minimum(slot + 1, capacity - 1)
            later_mask = wet_of(later)
            row = jnp.minimum(rows[spot + 1] + rank, capacity - 1)
            after = jnp.where(slot + 1 == length, right, received[row] * later_mask)
            low = pltpu.roll(jnp.where(at_last, before, here), 1, 1)
            high = pltpu.roll(jnp.where(at_first, after, here), cells - 1, 1)
            done[slot] = (low + high + 2.0 * here) * (scale * mask)
            return here, after, later_mask

        carry = lax.fori_loop(0, devices, one, carry, unroll=8)
        out_copy(rank).start()
        return carry

    mask = wet_of(jnp.int32(0))
    lax.fori_loop(0, pair_most, one_rank, (left, received[rows[0]] * mask, mask))

    @pl.loop(0, pair_most)
    def _(rank):
        out_copy(rank).wait()


def choose_kernel(sizes, main, spares, spans, out):
    groups, chips, layers = sizes
    devices = groups * chips
    plane = chips // layers
    over, most = [], jnp.int32(0)
    for layer in range(layers):
        need = jnp.int32(0)
        for grp in range(groups):
            part = jnp.int32(0)
            for spot in range(plane):
                part = part + spans[grp * chips + layer * plane + spot]
            part = lax.div(part + devices - 1, devices)
            if grp == 0:
                most = jnp.maximum(most, part)
            need = need + part
        over.append(jnp.maximum(need - main, 0))
    need = jnp.maximum(over[0] + over[1], over[2] + over[3])
    choice = jnp.int32(len(spares))
    for number, (spare, early) in reversed(list(enumerate(spares))):
        choice = jnp.where((need <= spare) & (most <= early), number, choice)
    out[0] = choice


def on_device(accum, step_count, stretch_slot, span_length, wet_mask):
    groups, chips = lax.axis_size("grp"), lax.axis_size("dev")
    devices = groups * chips
    blocks_dev, fields, cells = accum.shape
    capacity = wet_mask.shape[0]
    pair_most = capacity // devices
    all_blocks = stretch_slot.shape[0]
    layers = 4 if chips % 4 == 0 else 1
    smem = pl.BlockSpec(memory_space=pltpu.SMEM)
    vmem = pl.BlockSpec(memory_space=pltpu.VMEM)
    hbm = pl.BlockSpec(memory_space=pl.ANY)
    block = (fields, cells)
    f32 = jnp.float32
    sems = pltpu.SemaphoreType.DMA
    rows = pltpu.VMEM((capacity, *block), f32)
    pair = pltpu.VMEM((2, *block), f32)
    shapes = (
        jax.ShapeDtypeStruct((capacity, *block), f32),
        jax.ShapeDtypeStruct((2, *block), f32),
    )
    operands = (stretch_slot, span_length, wet_mask, accum)
    sizes = (groups, chips, layers, pair_most, blocks_dev, all_blocks)

    def exchange(kernel, scratch, number):
        return pl.pallas_call(
            kernel,
            out_shape=shapes,
            in_specs=[smem, smem, smem, vmem],
            out_specs=(hbm, hbm),
            scratch_shapes=scratch,
            compiler_params=pltpu.CompilerParams(collective_id=number, has_side_effects=True),
        )

    def direct(*given):
        scratch = [pltpu.SMEM((devices,), jnp.int32), rows, rows, pair, pair]
        scratch += [sems((devices,))] * 3 + [sems((2,)), sems((2,)), sems]
        return exchange(functools.partial(exchange_kernel, sizes), scratch, 0)(*given)

    def stream(number, spare, early):
        def run(*given):
            rests = devices // layers
            main = rests * pair_most // 2
            room = main + spare

            def many(*count):
                return pltpu.VMEM((*count, *block), f32)

            scratch = [pltpu.SMEM((devices + 1,), jnp.int32), many(blocks_dev), many(room + 1)]
            scratch += [many(spare + 1), many(main), many(main), many(3, room + 1), many(3, room)]
            scratch += [many(4 * rests * pair_most), many(), many(rests)]
            scratch += [sems, sems((2,)), sems((2,)), sems, sems((3,)), sems((3,))]
            scratch += [sems((2, 2)), sems((3, 2)), sems((4 * rests,)), sems((devices,))]
            scratch += [sems((rests,)), sems((rests,))]
            return pl.pallas_call(
                functools.partial(stream_kernel, sizes, spare, early),
                out_shape=shapes,
                in_specs=[smem, smem, smem, hbm],
                out_specs=(vmem, vmem),
                scratch_shapes=scratch,
                compiler_params=pltpu.CompilerParams(collective_id=number, has_side_effects=True),
            )(*given)

        return run

    ready = devices & (devices - 1) == 0 and 4 * devices <= cells
    if layers == 4 and groups == 2 and pair_most >= 8 and ready:
        main = (devices // layers) * pair_most // 2
        spares = [(main * spare // 32, main * early // 32) for spare, early in SPARES]
        choice = pl.pallas_call(
            functools.partial(choose_kernel, (groups, chips, layers), main, spares),
            out_shape=jax.ShapeDtypeStruct((1,), jnp.int32),
            in_specs=[smem],
            out_specs=smem,
        )(span_length)[0]
        branches = [stream(number + 1, *spare) for number, spare in enumerate(spares)] + [direct]
        received, halo = lax.switch(choice, branches, *operands)
    else:
        received, halo = direct(*operands)
    return pl.pallas_call(
        functools.partial(filter_kernel, (groups, chips, pair_most, blocks_dev, all_blocks)),
        out_shape=shapes[0],
        in_specs=[smem, smem, smem, smem, vmem, vmem],
        out_specs=hbm,
        scratch_shapes=[pltpu.SMEM((devices + 1,), jnp.int32), rows, sems((pair_most,))],
    )(stretch_slot, span_length, wet_mask, step_count, received, halo)


def solution(mesh):
    return jax.shard_map(
        on_device,
        mesh=mesh,
        in_specs=(P(("grp", "dev"), None, None), P(), P(), P(), P(("grp", "dev"))),
        out_specs=P(("grp", "dev"), None, None),
        check_vma=False,
    )
```

```python
import functools
import jax
import jax.numpy as jnp
from jax import lax
from jax.experimental import pallas as pl
from jax.experimental.pallas import tpu as pltpu
from jax.sharding import PartitionSpec as P

MESH = pl.DeviceIdType.MESH
SPARES = ((4, 24), (6, 24), (8, 24), (10, 24), (12, 24), (14, 24), (16, 24), (20, 24), (12, 32), (20, 32), (32, 32))


def exchange_kernel(
    sizes, stretch, spans, wet, accum, received, halo,
    starts, packed, landed, edge_out, edge_in, send_sem, recv_sem, out_sem, edge_send, edge_recv, edge_copy,
):
    groups, chips, layers, pair_most, blocks_dev, all_blocks = sizes
    devices = groups * chips
    plane = chips // layers
    grp = lax.axis_index("grp")
    dev = lax.axis_index("dev")
    me = grp * chips + dev
    layer, place = dev // plane, dev % plane

    def at(index):
        return (index // chips, index % chips)

    barrier = pltpu.get_barrier_semaphore()

    @pl.loop(1, devices)
    def _(step):
        pl.semaphore_signal(barrier, inc=1, device_id=at((me + step) % devices), device_id_type=MESH)

    def prefix(owner, total):
        starts[owner] = total
        return total + spans[owner]

    lax.fori_loop(0, devices, prefix, jnp.int32(0))

    def find(block, found):
        return jnp.where(stretch[block] // blocks_dev == me, block, found)

    phase = lax.fori_loop(0, devices, find, jnp.int32(0), unroll=8)

    def partner(turn, rest):
        there = ((layer + turn) % layers) * plane + (place + rest % plane) % plane
        return ((grp + rest // plane) % groups) * chips + there

    def pack(owner, target, base):
        start = starts[owner]
        first = start + lax.rem(phase - start + all_blocks * devices, devices)
        for rank in range(pair_most):
            block = jnp.minimum(first + rank * devices, all_blocks - 1)
            slot = lax.rem(stretch[block], blocks_dev)
            target[base + rank] = accum[slot]

    def send_copy(other):
        return pltpu.make_async_remote_copy(
            src_ref=packed.at[pl.ds(other * pair_most, pair_most)],
            dst_ref=landed.at[pl.ds(me * pair_most, pair_most)],
            send_sem=send_sem.at[other],
            recv_sem=recv_sem.at[me],
            device_id=at(other),
            device_id_type=MESH,
        )

    def out_copy(other):
        return pltpu.make_async_copy(
            landed.at[pl.ds(other * pair_most, pair_most)],
            received.at[pl.ds(other * pair_most, pair_most)],
            out_sem.at[other],
        )

    turns = [layers // 2] + [t for t in range(1, layers) if t != layers // 2]
    if layers > 1:
        turns = turns + [0]
    else:
        turns = [0]
    rests = groups * plane
    for number, turn in enumerate(turns):
        low = 1 if turn == 0 else 0

        @pl.loop(low, rests)
        def _(rest):
            other = partner(turn, rest)
            pack(other, packed, other * pair_most)

        if number == 0:
            pl.semaphore_wait(barrier, devices - 1)

        @pl.loop(low, rests)
        def _(rest):
            send_copy(partner(turn, rest)).start()

    pack(me, landed, me * pair_most)

    for turn in reversed(turns):
        low = 1 if turn == 0 else 0

        @pl.loop(low, rests)
        def _(rest):
            other = partner(turn, rest)
            pltpu.make_async_remote_copy(
                src_ref=packed.at[pl.ds(other * pair_most, pair_most)],
                dst_ref=landed.at[pl.ds(other * pair_most, pair_most)],
                send_sem=send_sem.at[other],
                recv_sem=recv_sem.at[other],
                device_id=at(other),
                device_id_type=MESH,
            ).wait_recv()
            out_copy(other).start()

    out_copy(me).start()

    start = starts[me]
    length = spans[me]
    first_from = stretch[start] // blocks_dev
    last = jnp.maximum(length - 1, 0)
    last_from = stretch[start + last] // blocks_dev
    edge_out[0] = landed[last_from * pair_most + last // devices] * (
        wet[last] == 1
    ).astype(jnp.float32)
    edge_out[1] = landed[first_from * pair_most] * (wet[0] == 1).astype(jnp.float32)
    copies = []
    for side, shift in ((0, 1), (1, devices - 1)):
        copies.append(
            pltpu.make_async_remote_copy(
                src_ref=edge_out.at[side],
                dst_ref=edge_in.at[side],
                send_sem=edge_send.at[side],
                recv_sem=edge_recv.at[side],
                device_id=at((me + shift) % devices),
                device_id_type=MESH,
            )
        )
    for copy in copies:
        copy.start()

    @pl.loop(1, devices)
    def _(step):
        send_copy((me + step) % devices).wait_send()

    @pl.loop(0, devices)
    def _(other):
        out_copy(other).wait()

    for copy in copies:
        copy.wait()
    final = pltpu.make_async_copy(edge_in, halo, edge_copy)
    final.start()
    final.wait()


def stream_kernel(
    sizes, spare, early, stretch, spans, wet, accum_at, received, halo,
    starts, accum, to_mate, to_spare, to_near, to_far, lists, merged, forward, edge_all, edge_near,
    load_sem, mate_send, mate_recv, spare_send, spare_recv, pass_send, main_send, main_recv,
    near_send, near_recv, edge_send, edge_recv,
):
    groups, chips, layers, pair_most, blocks_dev, all_blocks = sizes
    devices = groups * chips
    plane = chips // layers
    rests = groups * plane
    main = rests * pair_most // 2
    room = main + spare
    _, fields, cells = accum.shape
    shift = devices.bit_length() - 1
    grp = lax.axis_index("grp")
    dev = lax.axis_index("dev")
    me = grp * chips + dev
    layer, place = dev // plane, dev % plane
    low = layer < 2
    inner = (layer == 1) | (layer == 2)
    across = (
        layer, layer + 1 - 2 * (layer % 2), jnp.where(low, 2, 1), jnp.where(low, 3, 0)
    )
    my_spot = grp * plane + place

    def at(index):
        return (index // chips, index % chips)

    def column(there):
        return grp * chips + there * plane + place

    def mate(spot):
        return (spot // plane) * chips + layer * plane + spot % plane

    load = pltpu.make_async_copy(accum_at, accum, load_sem)
    load.start()
    barrier = pltpu.get_barrier_semaphore()
    for turn in (1, 2, 3):
        pl.semaphore_signal(
            barrier, inc=1, device_id=at(column((layer + turn) % layers)), device_id_type=MESH
        )

    @pl.loop(1, rests)
    def _(step):
        pl.semaphore_signal(
            barrier, inc=1, device_id=at(mate((my_spot + step) % rests)), device_id_type=MESH
        )

    def prefix(owner, total):
        starts[owner] = total
        return total + spans[owner]

    starts[devices] = lax.fori_loop(0, devices, prefix, jnp.int32(0), unroll=8)

    def find(block, found):
        holder = lax.div(stretch[block], blocks_dev)
        return tuple(
            jnp.where(holder == column(across[turn]), block, found[turn]) for turn in range(4)
        )

    phases = lax.fori_loop(0, devices, find, (jnp.int32(0),) * 4, unroll=8)

    def rank_of(phase, owner):
        return lax.shift_right_arithmetic(starts[owner] + (devices - 1) - phase, jnp.int32(shift))

    def layer_list(phase, there):
        marks = []
        for part in range(2):
            first = part * chips + there * plane
            begin = rank_of(phase, first)
            marks.append((begin, rank_of(phase, first + plane) - begin))
        (begin_low, amount), (begin_high, more) = marks
        return amount, begin_low, begin_high - amount, amount + more

    def slot_of(rank, phase):
        block = jnp.minimum(phase + rank * devices, all_blocks - 1)
        return lax.rem(stretch[block], blocks_dev)

    mine = phases[0]
    lists_to = [layer_list(mine, across[turn]) for turn in range(4)]

    def block_at(listed, spot):
        amount, begin_low, begin_high, _ = listed
        return accum[slot_of(spot + jnp.where(spot < amount, begin_low, begin_high), mine)]

    def fill(target, begin, end, listed):
        def one(spot, carry):
            target[spot] = block_at(listed, spot)
            return carry

        lax.fori_loop(begin, end, one, jnp.int32(0), unroll=4)

    far_list = jnp.where(inner, 1, 2)

    def pick(turn, values):
        if turn == "first":
            return jnp.where(inner, values[2], values[3])
        if turn == "second":
            return jnp.where(inner, values[3], values[2])
        return values[turn]

    def order(turn):
        return {"first": 2, "second": 3}.get(turn, turn)

    def mate_copy(step):
        begin, end = ((0, early), (early, room + 1))[step]
        return pltpu.make_async_remote_copy(
            src_ref=to_mate.at[pl.ds(begin, end - begin)],
            dst_ref=lists.at[0, pl.ds(begin, end - begin)],
            send_sem=mate_send.at[step],
            recv_sem=mate_recv.at[step],
            device_id=at(column(across[1])),
            device_id_type=MESH,
        )

    def spare_copy(where):
        return pltpu.make_async_remote_copy(
            src_ref=to_spare,
            dst_ref=lists.at[where, pl.ds(main, spare + 1)],
            send_sem=spare_send,
            recv_sem=spare_recv.at[where],
            device_id=at(column(across[2])),
            device_id_type=MESH,
        )

    def pass_copy(where):
        return pltpu.make_async_remote_copy(
            src_ref=lists.at[where, pl.ds(main, spare + 1)],
            dst_ref=lists.at[where, pl.ds(main, spare + 1)],
            send_sem=pass_send.at[where],
            recv_sem=spare_recv.at[where],
            device_id=at(column(across[1])),
            device_id_type=MESH,
        )

    third = main // 2
    cuts = [(0, third), (third, early), (early, main)] if early < main else [(0, third), (third, main)]
    last = len(cuts) - 1
    stops = [plane // 2, plane, rests] if early < main else [plane // 2, rests]
    groups_of = list(zip([0] + stops[:-1], stops, [end for _, end in cuts[:-1]] + [room]))

    def main_copy(outer, step, where):
        begin, end = cuts[step]
        return pltpu.make_async_remote_copy(
            src_ref=(to_far if outer else to_near).at[pl.ds(begin, end - begin)],
            dst_ref=lists.at[where, pl.ds(begin, end - begin)],
            send_sem=main_send.at[outer, step],
            recv_sem=main_recv.at[where, step],
            device_id=at(column(across[3 if outer else 2])),
            device_id_type=MESH,
        )

    def near_copy(turn, spot, sender):
        return pltpu.make_async_remote_copy(
            src_ref=forward.at[pl.ds((order(turn) * rests + spot) * pair_most, pair_most)],
            dst_ref=received.at[pl.ds(sender * pair_most, pair_most)],
            send_sem=near_send.at[order(turn) * rests + spot],
            recv_sem=near_recv.at[sender],
            device_id=at(mate(spot)),
            device_id_type=MESH,
        )

    def edge_copy(spot, sender):
        return pltpu.make_async_remote_copy(
            src_ref=edge_all,
            dst_ref=edge_near.at[sender],
            send_sem=edge_send.at[spot],
            recv_sem=edge_recv.at[sender],
            device_id=at(mate(spot)),
            device_id_type=MESH,
        )

    def hand_on(turn, begin, end, limit):
        listed = pick(turn, (0, 0, 1, 2))
        phase = pick(turn, phases)
        sender = column(pick(turn, across))
        if turn != 0:
            amount, begin_low, begin_high, _ = layer_list(phase, layer)
            jump = jnp.int32(0)
            if turn != 1:
                other = layer_list(phase, across[1])[3]
                jump = jnp.where(inner, jnp.maximum(other - main, 0), 0)

        def put(spot, target, base):
            owner = mate(spot)
            first = rank_of(phase, owner)
            if turn != 0:
                first = first - jnp.where(spot < plane, begin_low, begin_high)
            for step in range(pair_most):
                if turn == 0:
                    target[base + step] = accum[slot_of(first + step, phase)]
                else:
                    row = first + step
                    if turn != 1:
                        row = row + jnp.where(row < main, 0, jump)
                    target[base + step] = merged[listed, jnp.clip(row, 0, limit - 1)]

        @pl.loop(begin, end)
        def _(spot):
            @pl.when(spot != my_spot)
            def _():
                put(spot, forward, (order(turn) * rests + spot) * pair_most)

            @pl.when(spot == my_spot)
            def _():
                put(spot, received, sender * pair_most)

        @pl.loop(begin, end)
        def _(spot):
            @pl.when(spot != my_spot)
            def _():
                near_copy(turn, spot, sender).start()

    load.wait()
    fill(to_mate, 0, early, lists_to[1])

    @pl.when(inner)
    def _():
        fill(to_far, 0, cuts[last][0], lists_to[3])

    pl.semaphore_wait(barrier, layers - 1 + rests - 1)
    mate_copy(0).start()

    @pl.when(inner)
    def _():
        for step in range(last):
            main_copy(1, step, far_list).start()

    hand_on(0, 0, rests, None)

    lane = lax.broadcasted_iota(jnp.int32, (fields, cells), 1)
    ending = jnp.maximum(spans[me] - 1, 0)
    edges = jnp.where(
        lane == 2 * (devices + me),
        jnp.where(wet[0] == 1, 1.0, 0.0),
        jnp.where(
            lane == 2 * (devices + me) + 1, jnp.where(wet[ending] == 1, 1.0, 0.0), 0.0
        ),
    )

    def collect(owner, edges):
        for back, turned in ((1, 2 * owner), (0, 2 * owner - 1)):
            held = stretch[jnp.clip(starts[owner] - back, 0, all_blocks - 1)]
            rolled = pltpu.roll(accum[lax.rem(held, blocks_dev)], (turned + back) % cells, 1)
            wanted = jnp.where(lax.div(held, blocks_dev) == me, turned, -1)
            edges = jnp.where(lane == wanted, rolled, edges)
        return edges

    edges = lax.fori_loop(1, devices, collect, edges, unroll=2)
    to_mate[room] = edges
    to_spare[spare] = edges
    over = jnp.maximum(lists_to[3][3] - main, 0)

    def fill_spare(spot, carry):
        rank = []
        for listed, back in ((lists_to[3], 0), (lists_to[2], over)):
            amount, begin_low, begin_high, _ = listed
            there = main + spot - back
            rank.append(there + jnp.where(there < amount, begin_low, begin_high))
        to_spare[spot] = accum[slot_of(jnp.where(spot < over, rank[0], rank[1]), mine)]
        return carry

    lax.fori_loop(0, spare, fill_spare, jnp.int32(0), unroll=2)
    fill(to_mate, early, room, lists_to[1])
    spare_copy(far_list).start()
    mate_copy(1).start()
    last = len(cuts) - 1

    @pl.when(inner)
    def _():
        fill(to_near, 0, main, lists_to[2])
        for step in range(last):
            main_copy(0, step, far_list).start()
        fill(to_far, *cuts[last], lists_to[3])
        main_copy(1, last, far_list).start()
        main_copy(0, last, far_list).start()

    @pl.when(jnp.logical_not(inner))
    def _():
        for step in range(last + 1):
            fill(to_far, *cuts[step], lists_to[3])
            fill(to_near, *cuts[step], lists_to[2])
            main_copy(1, step, far_list).start()
            main_copy(0, step, far_list).start()

    def merge(where, begin, end):
        part = pl.ds(begin, end - begin)
        merged[where, part] = lists[where, part]

    def arrive(where, step):
        main_copy(0, step, where).wait_recv()
        merge(where, *cuts[step])

    def spared(where):
        spare_copy(where).wait_recv()
        merge(where, main, room)

    def advance(where, step):
        arrive(where, step)
        hand_on(where + 1, *groups_of[step])

    def sum_edges():
        total = edges
        for where in range(3):
            total = total + lists[where, room]
        edge_all[...] = total

        @pl.loop(0, rests)
        def _(spot):
            @pl.when(spot != my_spot)
            def _():
                edge_copy(spot, my_spot).start()

    @pl.when(inner)
    def _():
        spared(1)
        pass_copy(1).start()
        spared(2)
        pass_copy(2).start()

    mate_copy(0).wait_recv()
    merge(0, 0, early)
    hand_on(1, 0, plane, early)

    @pl.when(jnp.logical_not(inner))
    def _():
        for step in range(last):
            advance(1, step)

    mate_copy(1).wait_recv()
    merge(0, early, room)
    hand_on(1, plane, rests, room)

    @pl.when(inner)
    def _():
        sum_edges()

    for step in range(last):
        advance(2, step)

    @pl.when(jnp.logical_not(inner))
    def _():
        spared(2)
        spared(1)
        sum_edges()

    advance(2, last)

    @pl.when(inner)
    def _():
        for step in range(last):
            advance(1, step)

    advance(1, last)

    @pl.when(inner)
    def _():
        for where in (1, 2):
            pass_copy(where).wait_send()

    for step in range(2):
        mate_copy(step).wait_send()
    spare_copy(far_list).wait_send()
    for outer in range(2):
        for step in range(last + 1):
            main_copy(outer, step, far_list).wait_send()

    edge_near[my_spot] = edge_all[...]

    @pl.loop(0, rests)
    def _(spot):
        @pl.when(spot != my_spot)
        def _():
            edge_copy(spot, spot).wait()

    total = edge_near[0]
    for spot in range(1, rests):
        total = total + edge_near[spot]
    spread = cells * devices

    def cell(to, lane_from):
        return pltpu.roll(total, lax.rem(to - lane_from + spread, cells), 1)

    wet_left, wet_right = 2 * (devices + me) - 1, 2 * (devices + me) + 2
    halo[0] = cell(cells - 1, 2 * me) * cell(cells - 1, wet_left)
    halo[1] = cell(0, 2 * me + 1) * cell(0, wet_right)

    @pl.loop(0, rests)
    def _(spot):
        @pl.when(spot != my_spot)
        def _():
            for turn in range(4):
                sender = (spot // plane) * chips + across[turn] * plane + spot % plane
                near_copy(turn, spot, sender).wait()


def filter_kernel(sizes, stretch, spans, wet, counts, received, halo, out, rows, done, sem):
    groups, chips, pair_most, blocks_dev, all_blocks = sizes
    devices = groups * chips
    me = lax.axis_index("grp") * chips + lax.axis_index("dev")
    length = spans[me]
    capacity = wet.shape[0]
    _, fields, cells = halo.shape
    start = lax.fori_loop(
        0, devices, lambda o, s: s + jnp.where(o < me, spans[o], 0), jnp.int32(0), unroll=8
    )

    def fill(spot, carry):
        block = jnp.minimum(start + spot, all_blocks - 1)
        rows[spot] = lax.div(stretch[block], blocks_dev) * pair_most
        return carry

    lax.fori_loop(0, devices, fill, jnp.int32(0), unroll=8)
    rows[devices] = rows[0] + 1
    field = lax.broadcasted_iota(jnp.int32, (fields, cells), 0)
    held = jnp.ones((fields, cells), jnp.int32)
    for index in range(fields):
        held = jnp.where(field == index, counts[index], held)
    scale = 0.25 / held.astype(jnp.float32)
    lane = lax.broadcasted_iota(jnp.int32, (fields, cells), 1)
    at_first, at_last = lane == 0, lane == cells - 1
    left = halo[0] * jnp.where(me > 0, 1.0, 0.0)
    right = halo[1] * jnp.where(me < devices - 1, 1.0, 0.0)

    def wet_of(slot):
        return jnp.where(slot < length, wet[slot], 0).astype(jnp.float32)

    def out_copy(rank):
        part = pl.ds(rank * devices, devices)
        return pltpu.make_async_copy(done.at[part], out.at[part], sem.at[rank])

    def one_rank(rank, carry):
        def one(spot, carry):
            before, here, mask = carry
            slot = rank * devices + spot
            later = jnp.minimum(slot + 1, capacity - 1)
            later_mask = wet_of(later)
            row = jnp.minimum(rows[spot + 1] + rank, capacity - 1)
            after = jnp.where(slot + 1 == length, right, received[row] * later_mask)
            low = pltpu.roll(jnp.where(at_last, before, here), 1, 1)
            high = pltpu.roll(jnp.where(at_first, after, here), cells - 1, 1)
            done[slot] = (low + high + 2.0 * here) * (scale * mask)
            return here, after, later_mask

        carry = lax.fori_loop(0, devices, one, carry, unroll=min(devices, 32))
        out_copy(rank).start()
        return carry

    mask = wet_of(jnp.int32(0))
    lax.fori_loop(0, pair_most, one_rank, (left, received[rows[0]] * mask, mask))

    @pl.loop(0, pair_most)
    def _(rank):
        out_copy(rank).wait()


def choose_kernel(sizes, main, spares, spans, out):
    groups, chips, layers = sizes
    devices = groups * chips
    plane = chips // layers
    over, most = [], jnp.int32(0)
    for layer in range(layers):
        need = jnp.int32(0)
        for grp in range(groups):
            part = jnp.int32(0)
            for spot in range(plane):
                part = part + spans[grp * chips + layer * plane + spot]
            part = lax.div(part + devices - 1, devices)
            if grp == 0:
                most = jnp.maximum(most, part)
            need = need + part
        over.append(jnp.maximum(need - main, 0))
    need = jnp.maximum(over[0] + over[1], over[2] + over[3])
    choice = jnp.int32(len(spares))
    for number, (spare, early) in reversed(list(enumerate(spares))):
        choice = jnp.where((need <= spare) & (most <= early), number, choice)
    out[0] = choice


def on_device(accum, step_count, stretch_slot, span_length, wet_mask):
    groups, chips = lax.axis_size("grp"), lax.axis_size("dev")
    devices = groups * chips
    blocks_dev, fields, cells = accum.shape
    capacity = wet_mask.shape[0]
    pair_most = capacity // devices
    all_blocks = stretch_slot.shape[0]
    layers = 4 if chips % 4 == 0 else 1
    smem = pl.BlockSpec(memory_space=pltpu.SMEM)
    vmem = pl.BlockSpec(memory_space=pltpu.VMEM)
    hbm = pl.BlockSpec(memory_space=pl.ANY)
    block = (fields, cells)
    f32 = jnp.float32
    sems = pltpu.SemaphoreType.DMA
    rows = pltpu.VMEM((capacity, *block), f32)
    pair = pltpu.VMEM((2, *block), f32)
    shapes = (
        jax.ShapeDtypeStruct((capacity, *block), f32),
        jax.ShapeDtypeStruct((2, *block), f32),
    )
    operands = (stretch_slot, span_length, wet_mask, accum)
    sizes = (groups, chips, layers, pair_most, blocks_dev, all_blocks)

    def exchange(kernel, scratch, number):
        return pl.pallas_call(
            kernel,
            out_shape=shapes,
            in_specs=[smem, smem, smem, vmem],
            out_specs=(hbm, hbm),
            scratch_shapes=scratch,
            compiler_params=pltpu.CompilerParams(collective_id=number, has_side_effects=True),
        )

    def direct(*given):
        scratch = [pltpu.SMEM((devices,), jnp.int32), rows, rows, pair, pair]
        scratch += [sems((devices,))] * 3 + [sems((2,)), sems((2,)), sems]
        return exchange(functools.partial(exchange_kernel, sizes), scratch, 0)(*given)

    def stream(number, spare, early):
        def run(*given):
            rests = devices // layers
            main = rests * pair_most // 2
            room = main + spare

            def many(*count):
                return pltpu.VMEM((*count, *block), f32)

            scratch = [pltpu.SMEM((devices + 1,), jnp.int32), many(blocks_dev), many(room + 1)]
            scratch += [many(spare + 1), many(main), many(main), many(3, room + 1), many(3, room)]
            scratch += [many(4 * rests * pair_most), many(), many(rests)]
            scratch += [sems, sems((2,)), sems((2,)), sems, sems((3,)), sems((3,))]
            scratch += [sems((2, 3)), sems((3, 3)), sems((4 * rests,)), sems((devices,))]
            scratch += [sems((rests,)), sems((rests,))]
            return pl.pallas_call(
                functools.partial(stream_kernel, sizes, spare, early),
                out_shape=shapes,
                in_specs=[smem, smem, smem, hbm],
                out_specs=(vmem, vmem),
                scratch_shapes=scratch,
                compiler_params=pltpu.CompilerParams(collective_id=number, has_side_effects=True),
            )(*given)

        return run

    ready = devices & (devices - 1) == 0 and 4 * devices <= cells
    if layers == 4 and groups == 2 and pair_most >= 8 and ready:
        main = (devices // layers) * pair_most // 2
        spares = [(main * spare // 32, main * early // 32) for spare, early in SPARES]
        choice = pl.pallas_call(
            functools.partial(choose_kernel, (groups, chips, layers), main, spares),
            out_shape=jax.ShapeDtypeStruct((1,), jnp.int32),
            in_specs=[smem],
            out_specs=smem,
        )(span_length)[0]
        branches = [stream(number + 1, *spare) for number, spare in enumerate(spares)] + [direct]
        received, halo = lax.switch(choice, branches, *operands)
    else:
        received, halo = direct(*operands)
    return pl.pallas_call(
        functools.partial(filter_kernel, (groups, chips, pair_most, blocks_dev, all_blocks)),
        out_shape=shapes[0],
        in_specs=[smem, smem, smem, smem, vmem, vmem],
        out_specs=hbm,
        scratch_shapes=[pltpu.SMEM((devices + 1,), jnp.int32), rows, sems((pair_most,))],
    )(stretch_slot, span_length, wet_mask, step_count, received, halo)


def solution(mesh):
    return jax.shard_map(
        on_device,
        mesh=mesh,
        in_specs=(P(("grp", "dev"), None, None), P(), P(), P(), P(("grp", "dev"))),
        out_specs=P(("grp", "dev"), None, None),
        check_vma=False,
    )
```

```python
import functools
import jax
import jax.numpy as jnp
from jax import lax
from jax.experimental import pallas as pl
from jax.experimental.pallas import tpu as pltpu
from jax.sharding import PartitionSpec as P

MESH = pl.DeviceIdType.MESH
SPARES = ((4, 24), (6, 24), (8, 24), (10, 24), (12, 24), (14, 24), (16, 24), (20, 24), (12, 28), (20, 28), (32, 32))


def exchange_kernel(
    sizes, stretch, spans, wet, accum, received, halo,
    starts, packed, landed, edge_out, edge_in, send_sem, recv_sem, out_sem, edge_send, edge_recv, edge_copy,
):
    groups, chips, layers, pair_most, blocks_dev, all_blocks = sizes
    devices = groups * chips
    plane = chips // layers
    grp = lax.axis_index("grp")
    dev = lax.axis_index("dev")
    me = grp * chips + dev
    layer, place = dev // plane, dev % plane

    def at(index):
        return (index // chips, index % chips)

    barrier = pltpu.get_barrier_semaphore()

    @pl.loop(1, devices)
    def _(step):
        pl.semaphore_signal(barrier, inc=1, device_id=at((me + step) % devices), device_id_type=MESH)

    def prefix(owner, total):
        starts[owner] = total
        return total + spans[owner]

    lax.fori_loop(0, devices, prefix, jnp.int32(0))

    def find(block, found):
        return jnp.where(stretch[block] // blocks_dev == me, block, found)

    phase = lax.fori_loop(0, devices, find, jnp.int32(0), unroll=8)

    def partner(turn, rest):
        there = ((layer + turn) % layers) * plane + (place + rest % plane) % plane
        return ((grp + rest // plane) % groups) * chips + there

    def pack(owner, target, base):
        start = starts[owner]
        first = start + lax.rem(phase - start + all_blocks * devices, devices)
        for rank in range(pair_most):
            block = jnp.minimum(first + rank * devices, all_blocks - 1)
            slot = lax.rem(stretch[block], blocks_dev)
            target[base + rank] = accum[slot]

    def send_copy(other):
        return pltpu.make_async_remote_copy(
            src_ref=packed.at[pl.ds(other * pair_most, pair_most)],
            dst_ref=landed.at[pl.ds(me * pair_most, pair_most)],
            send_sem=send_sem.at[other],
            recv_sem=recv_sem.at[me],
            device_id=at(other),
            device_id_type=MESH,
        )

    def out_copy(other):
        return pltpu.make_async_copy(
            landed.at[pl.ds(other * pair_most, pair_most)],
            received.at[pl.ds(other * pair_most, pair_most)],
            out_sem.at[other],
        )

    turns = [layers // 2] + [t for t in range(1, layers) if t != layers // 2]
    if layers > 1:
        turns = turns + [0]
    else:
        turns = [0]
    rests = groups * plane
    for number, turn in enumerate(turns):
        low = 1 if turn == 0 else 0

        @pl.loop(low, rests)
        def _(rest):
            other = partner(turn, rest)
            pack(other, packed, other * pair_most)

        if number == 0:
            pl.semaphore_wait(barrier, devices - 1)

        @pl.loop(low, rests)
        def _(rest):
            send_copy(partner(turn, rest)).start()

    pack(me, landed, me * pair_most)

    for turn in reversed(turns):
        low = 1 if turn == 0 else 0

        @pl.loop(low, rests)
        def _(rest):
            other = partner(turn, rest)
            pltpu.make_async_remote_copy(
                src_ref=packed.at[pl.ds(other * pair_most, pair_most)],
                dst_ref=landed.at[pl.ds(other * pair_most, pair_most)],
                send_sem=send_sem.at[other],
                recv_sem=recv_sem.at[other],
                device_id=at(other),
                device_id_type=MESH,
            ).wait_recv()
            out_copy(other).start()

    out_copy(me).start()

    start = starts[me]
    length = spans[me]
    first_from = stretch[start] // blocks_dev
    last = jnp.maximum(length - 1, 0)
    last_from = stretch[start + last] // blocks_dev
    edge_out[0] = landed[last_from * pair_most + last // devices] * (
        wet[last] == 1
    ).astype(jnp.float32)
    edge_out[1] = landed[first_from * pair_most] * (wet[0] == 1).astype(jnp.float32)
    copies = []
    for side, shift in ((0, 1), (1, devices - 1)):
        copies.append(
            pltpu.make_async_remote_copy(
                src_ref=edge_out.at[side],
                dst_ref=edge_in.at[side],
                send_sem=edge_send.at[side],
                recv_sem=edge_recv.at[side],
                device_id=at((me + shift) % devices),
                device_id_type=MESH,
            )
        )
    for copy in copies:
        copy.start()

    @pl.loop(1, devices)
    def _(step):
        send_copy((me + step) % devices).wait_send()

    @pl.loop(0, devices)
    def _(other):
        out_copy(other).wait()

    for copy in copies:
        copy.wait()
    final = pltpu.make_async_copy(edge_in, halo, edge_copy)
    final.start()
    final.wait()


def stream_kernel(
    sizes, spare, early, stretch, spans, wet, accum_at, received, halo,
    starts, accum, to_mate, to_spare, to_near, to_far, lists, merged, forward, edge_all, edge_near,
    load_sem, mate_send, mate_recv, spare_send, spare_recv, pass_send, main_send, main_recv,
    near_send, near_recv, edge_send, edge_recv,
):
    groups, chips, layers, pair_most, blocks_dev, all_blocks = sizes
    devices = groups * chips
    plane = chips // layers
    rests = groups * plane
    main = rests * pair_most // 2
    room = main + spare
    _, fields, cells = accum.shape
    shift = devices.bit_length() - 1
    grp = lax.axis_index("grp")
    dev = lax.axis_index("dev")
    me = grp * chips + dev
    layer, place = dev // plane, dev % plane
    low = layer < 2
    inner = (layer == 1) | (layer == 2)
    across = (
        layer, layer + 1 - 2 * (layer % 2), jnp.where(low, 2, 1), jnp.where(low, 3, 0)
    )
    my_spot = grp * plane + place

    def at(index):
        return (index // chips, index % chips)

    def column(there):
        return grp * chips + there * plane + place

    def mate(spot):
        return (spot // plane) * chips + layer * plane + spot % plane

    load = pltpu.make_async_copy(accum_at, accum, load_sem)
    load.start()
    barrier = pltpu.get_barrier_semaphore()
    for turn in (1, 2, 3):
        pl.semaphore_signal(
            barrier, inc=1, device_id=at(column((layer + turn) % layers)), device_id_type=MESH
        )

    @pl.loop(1, rests)
    def _(step):
        pl.semaphore_signal(
            barrier, inc=1, device_id=at(mate((my_spot + step) % rests)), device_id_type=MESH
        )

    def prefix(owner, total):
        starts[owner] = total
        return total + spans[owner]

    starts[devices] = lax.fori_loop(0, devices, prefix, jnp.int32(0), unroll=8)

    def find(block, found):
        holder = lax.div(stretch[block], blocks_dev)
        return tuple(
            jnp.where(holder == column(across[turn]), block, found[turn]) for turn in range(4)
        )

    phases = lax.fori_loop(0, devices, find, (jnp.int32(0),) * 4, unroll=8)

    def rank_of(phase, owner):
        return lax.shift_right_arithmetic(starts[owner] + (devices - 1) - phase, jnp.int32(shift))

    def layer_list(phase, there):
        marks = []
        for part in range(2):
            first = part * chips + there * plane
            begin = rank_of(phase, first)
            marks.append((begin, rank_of(phase, first + plane) - begin))
        (begin_low, amount), (begin_high, more) = marks
        return amount, begin_low, begin_high - amount, amount + more

    def slot_of(rank, phase):
        block = jnp.minimum(phase + rank * devices, all_blocks - 1)
        return lax.rem(stretch[block], blocks_dev)

    mine = phases[0]
    lists_to = [layer_list(mine, across[turn]) for turn in range(4)]

    def block_at(listed, spot):
        amount, begin_low, begin_high, _ = listed
        return accum[slot_of(spot + jnp.where(spot < amount, begin_low, begin_high), mine)]

    def fill(target, begin, end, listed):
        def one(spot, carry):
            target[spot] = block_at(listed, spot)
            return carry

        lax.fori_loop(begin, end, one, jnp.int32(0), unroll=4)

    far_list = jnp.where(inner, 1, 2)

    def pick(turn, values):
        if turn == "first":
            return jnp.where(inner, values[2], values[3])
        if turn == "second":
            return jnp.where(inner, values[3], values[2])
        return values[turn]

    def order(turn):
        return {"first": 2, "second": 3}.get(turn, turn)

    def mate_copy(step):
        begin, end = ((0, early), (early, room + 1))[step]
        return pltpu.make_async_remote_copy(
            src_ref=to_mate.at[pl.ds(begin, end - begin)],
            dst_ref=lists.at[0, pl.ds(begin, end - begin)],
            send_sem=mate_send,
            recv_sem=mate_recv.at[step],
            device_id=at(column(across[1])),
            device_id_type=MESH,
        )

    def spare_copy(where):
        return pltpu.make_async_remote_copy(
            src_ref=to_spare,
            dst_ref=lists.at[where, pl.ds(main, spare + 1)],
            send_sem=spare_send,
            recv_sem=spare_recv.at[where - 1],
            device_id=at(column(across[2])),
            device_id_type=MESH,
        )

    def pass_copy(where):
        return pltpu.make_async_remote_copy(
            src_ref=lists.at[where, pl.ds(main, spare + 1)],
            dst_ref=lists.at[where, pl.ds(main, spare + 1)],
            send_sem=pass_send,
            recv_sem=spare_recv.at[where - 1],
            device_id=at(column(across[1])),
            device_id_type=MESH,
        )

    third = main // 2
    cuts = [(0, third), (third, early), (early, main)] if early < main else [(0, third), (third, main)]
    last = len(cuts) - 1
    stops = [plane // 2, plane, rests] if early < main else [plane // 2, rests]
    groups_of = list(zip([0] + stops[:-1], stops, [end for _, end in cuts[:-1]] + [room]))

    def main_copy(outer, step, where):
        begin, end = cuts[step]
        return pltpu.make_async_remote_copy(
            src_ref=(to_far if outer else to_near).at[pl.ds(begin, end - begin)],
            dst_ref=lists.at[where, pl.ds(begin, end - begin)],
            send_sem=main_send,
            recv_sem=main_recv.at[where - 1, step],
            device_id=at(column(across[3 if outer else 2])),
            device_id_type=MESH,
        )

    def near_copy(turn, spot, sender):
        return pltpu.make_async_remote_copy(
            src_ref=forward.at[pl.ds((order(turn) * rests + spot) * pair_most, pair_most)],
            dst_ref=received.at[pl.ds(sender * pair_most, pair_most)],
            send_sem=near_send,
            recv_sem=near_recv,
            device_id=at(mate(spot)),
            device_id_type=MESH,
        )

    def edge_copy(spot, sender):
        return pltpu.make_async_remote_copy(
            src_ref=edge_all,
            dst_ref=edge_near.at[sender],
            send_sem=edge_send,
            recv_sem=edge_recv,
            device_id=at(mate(spot)),
            device_id_type=MESH,
        )

    def whole(held, count, send_sem, recv_sem):
        part = held.at[pl.ds(0, count)]
        return pltpu.make_async_remote_copy(
            src_ref=part,
            dst_ref=part,
            send_sem=send_sem,
            recv_sem=recv_sem,
            device_id=at(column(across[1])),
            device_id_type=MESH,
        )

    def hand_on(turn, begin, end, limit):
        listed = pick(turn, (0, 0, 1, 2))
        phase = pick(turn, phases)
        sender = column(pick(turn, across))
        if turn != 0:
            amount, begin_low, begin_high, _ = layer_list(phase, layer)
            jump = jnp.int32(0)
            if turn != 1:
                other = layer_list(phase, across[1])[3]
                jump = jnp.where(inner, jnp.maximum(other - main, 0), 0)

        def put(spot, target, base):
            owner = mate(spot)
            first = rank_of(phase, owner)
            if turn != 0:
                first = first - jnp.where(spot < plane, begin_low, begin_high)
            for step in range(pair_most):
                if turn == 0:
                    target[base + step] = accum[slot_of(first + step, phase)]
                else:
                    row = first + step
                    if turn != 1:
                        row = row + jnp.where(row < main, 0, jump)
                    target[base + step] = merged[listed, jnp.clip(row, 0, limit - 1)]

        @pl.loop(begin, end)
        def _(spot):
            @pl.when(spot != my_spot)
            def _():
                put(spot, forward, (order(turn) * rests + spot) * pair_most)

            @pl.when(spot == my_spot)
            def _():
                put(spot, received, sender * pair_most)

        @pl.loop(begin, end)
        def _(spot):
            @pl.when(spot != my_spot)
            def _():
                near_copy(turn, spot, sender).start()

    load.wait()
    fill(to_mate, 0, early, lists_to[1])

    @pl.when(inner)
    def _():
        fill(to_far, 0, cuts[last][0], lists_to[3])

    pl.semaphore_wait(barrier, layers - 1 + rests - 1)
    mate_copy(0).start()

    @pl.when(inner)
    def _():
        for step in range(last):
            main_copy(1, step, far_list).start()

    hand_on(0, 0, rests, None)

    lane = lax.broadcasted_iota(jnp.int32, (fields, cells), 1)
    ending = jnp.maximum(spans[me] - 1, 0)
    edges = jnp.where(
        lane == 2 * (devices + me),
        jnp.where(wet[0] == 1, 1.0, 0.0),
        jnp.where(
            lane == 2 * (devices + me) + 1, jnp.where(wet[ending] == 1, 1.0, 0.0), 0.0
        ),
    )

    def collect(owner, edges):
        for back, turned in ((1, 2 * owner), (0, 2 * owner - 1)):
            held = stretch[jnp.clip(starts[owner] - back, 0, all_blocks - 1)]
            rolled = pltpu.roll(accum[lax.rem(held, blocks_dev)], (turned + back) % cells, 1)
            wanted = jnp.where(lax.div(held, blocks_dev) == me, turned, -1)
            edges = jnp.where(lane == wanted, rolled, edges)
        return edges

    edges = lax.fori_loop(1, devices, collect, edges, unroll=2)
    to_mate[room] = edges
    to_spare[spare] = edges
    over = jnp.maximum(lists_to[3][3] - main, 0)

    def fill_spare(spot, carry):
        rank = []
        for listed, back in ((lists_to[3], 0), (lists_to[2], over)):
            amount, begin_low, begin_high, _ = listed
            there = main + spot - back
            rank.append(there + jnp.where(there < amount, begin_low, begin_high))
        to_spare[spot] = accum[slot_of(jnp.where(spot < over, rank[0], rank[1]), mine)]
        return carry

    lax.fori_loop(0, spare, fill_spare, jnp.int32(0), unroll=2)
    fill(to_mate, early, room, lists_to[1])
    spare_copy(far_list).start()
    mate_copy(1).start()
    last = len(cuts) - 1

    @pl.when(inner)
    def _():
        fill(to_near, 0, main, lists_to[2])
        for step in range(last):
            main_copy(0, step, far_list).start()
        fill(to_far, *cuts[last], lists_to[3])
        main_copy(1, last, far_list).start()
        main_copy(0, last, far_list).start()

    @pl.when(jnp.logical_not(inner))
    def _():
        for step in range(last + 1):
            fill(to_near, *cuts[step], lists_to[2])
            fill(to_far, *cuts[step], lists_to[3])
            main_copy(0, step, far_list).start()
            main_copy(1, step, far_list).start()

    def merge(where, begin, end):
        part = pl.ds(begin, end - begin)
        merged[where, part] = lists[where, part]

    def arrive(where, step):
        main_copy(0, step, where).wait_recv()
        merge(where, *cuts[step])

    def spared(where):
        spare_copy(where).wait_recv()
        merge(where, main, room)

    def advance(where, step):
        arrive(where, step)
        hand_on(where + 1, *groups_of[step])

    def sum_edges():
        total = edges
        for where in range(3):
            total = total + lists[where, room]
        edge_all[...] = total

        @pl.loop(0, rests)
        def _(spot):
            @pl.when(spot != my_spot)
            def _():
                edge_copy(spot, my_spot).start()

    mate_copy(0).wait_recv()
    merge(0, 0, early)
    hand_on(1, 0, plane, early)

    @pl.when(inner)
    def _():
        spared(1)
        pass_copy(1).start()
        spared(2)
        pass_copy(2).start()

    @pl.when(jnp.logical_not(inner))
    def _():
        for step in range(last):
            advance(1, step)

    mate_copy(1).wait_recv()
    merge(0, early, room)
    hand_on(1, plane, rests, room)

    @pl.when(inner)
    def _():
        sum_edges()

    for step in range(last):
        advance(2, step)

    @pl.when(jnp.logical_not(inner))
    def _():
        spared(2)
        spared(1)
        sum_edges()

    advance(2, last)

    @pl.when(inner)
    def _():
        for step in range(last):
            advance(1, step)

    advance(1, last)

    @pl.when(inner)
    def _():
        whole(forward, 2 * (spare + 1), pass_send, near_recv).wait_send()

    whole(forward, room + 1, mate_send, near_recv).wait_send()
    spare_copy(far_list).wait_send()
    whole(forward, 2 * main, main_send, near_recv).wait_send()

    edge_near[my_spot] = edge_all[...]

    whole(edge_near, rests - 1, edge_send, edge_recv).wait()
    total = edge_near[0]
    for spot in range(1, rests):
        total = total + edge_near[spot]
    spread = cells * devices

    def cell(to, lane_from):
        return pltpu.roll(total, lax.rem(to - lane_from + spread, cells), 1)

    wet_left, wet_right = 2 * (devices + me) - 1, 2 * (devices + me) + 2
    halo[0] = cell(cells - 1, 2 * me) * cell(cells - 1, wet_left)
    halo[1] = cell(0, 2 * me + 1) * cell(0, wet_right)

    near_all = 4 * (rests - 1) * pair_most
    whole(forward, near_all, near_send, near_recv).wait_send()
    whole(received, near_all, near_send, near_recv).wait_recv()


def filter_kernel(sizes, stretch, spans, wet, counts, received, halo, out, rows, done, sem):
    groups, chips, pair_most, blocks_dev, all_blocks = sizes
    devices = groups * chips
    me = lax.axis_index("grp") * chips + lax.axis_index("dev")
    length = spans[me]
    capacity = wet.shape[0]
    _, fields, cells = halo.shape
    start = lax.fori_loop(
        0, devices, lambda o, s: s + jnp.where(o < me, spans[o], 0), jnp.int32(0), unroll=8
    )

    def fill(spot, carry):
        block = jnp.minimum(start + spot, all_blocks - 1)
        rows[spot] = lax.div(stretch[block], blocks_dev) * pair_most
        return carry

    lax.fori_loop(0, devices, fill, jnp.int32(0), unroll=8)
    rows[devices] = rows[0] + 1
    field = lax.broadcasted_iota(jnp.int32, (fields, cells), 0)
    held = jnp.ones((fields, cells), jnp.int32)
    for index in range(fields):
        held = jnp.where(field == index, counts[index], held)
    scale = 0.25 / held.astype(jnp.float32)
    lane = lax.broadcasted_iota(jnp.int32, (fields, cells), 1)
    at_first, at_last = lane == 0, lane == cells - 1
    left = halo[0] * jnp.where(me > 0, 1.0, 0.0)
    right = halo[1] * jnp.where(me < devices - 1, 1.0, 0.0)

    def wet_of(slot):
        return jnp.where(slot < length, wet[slot], 0).astype(jnp.float32)

    def out_copy(rank):
        part = pl.ds(rank * devices, devices)
        return pltpu.make_async_copy(done.at[part], out.at[part], sem)

    def one_rank(rank, carry):
        def one(spot, carry):
            before, here, mask = carry
            slot = rank * devices + spot
            later = jnp.minimum(slot + 1, capacity - 1)
            later_mask = wet_of(later)
            row = jnp.minimum(rows[spot + 1] + rank, capacity - 1)
            after = jnp.where(slot + 1 == length, right, received[row] * later_mask)
            low = pltpu.roll(jnp.where(at_last, before, here), 1, 1)
            high = pltpu.roll(jnp.where(at_first, after, here), cells - 1, 1)
            done[slot] = (low + high + 2.0 * here) * (scale * mask)
            return here, after, later_mask

        carry = lax.fori_loop(0, devices, one, carry, unroll=min(devices, 32))
        out_copy(rank).start()
        return carry

    mask = wet_of(jnp.int32(0))
    lax.fori_loop(0, pair_most, one_rank, (left, received[rows[0]] * mask, mask))

    pltpu.make_async_copy(done, out, sem).wait()


def choose_kernel(sizes, main, spares, spans, out):
    groups, chips, layers = sizes
    devices = groups * chips
    plane = chips // layers
    over, most = [], jnp.int32(0)
    for layer in range(layers):
        need = jnp.int32(0)
        for grp in range(groups):
            part = jnp.int32(0)
            for spot in range(plane):
                part = part + spans[grp * chips + layer * plane + spot]
            part = lax.div(part + devices - 1, devices)
            if grp == 0:
                most = jnp.maximum(most, part)
            need = need + part
        over.append(jnp.maximum(need - main, 0))
    need = jnp.maximum(over[0] + over[1], over[2] + over[3])
    choice = jnp.int32(len(spares))
    for number, (spare, early) in reversed(list(enumerate(spares))):
        choice = jnp.where((need <= spare) & (most <= early), number, choice)
    out[0] = choice


def on_device(accum, step_count, stretch_slot, span_length, wet_mask):
    groups, chips = lax.axis_size("grp"), lax.axis_size("dev")
    devices = groups * chips
    blocks_dev, fields, cells = accum.shape
    capacity = wet_mask.shape[0]
    pair_most = capacity // devices
    all_blocks = stretch_slot.shape[0]
    layers = 4 if chips % 4 == 0 else 1
    smem = pl.BlockSpec(memory_space=pltpu.SMEM)
    vmem = pl.BlockSpec(memory_space=pltpu.VMEM)
    hbm = pl.BlockSpec(memory_space=pl.ANY)
    block = (fields, cells)
    f32 = jnp.float32
    sems = pltpu.SemaphoreType.DMA
    rows = pltpu.VMEM((capacity, *block), f32)
    pair = pltpu.VMEM((2, *block), f32)
    shapes = (
        jax.ShapeDtypeStruct((capacity, *block), f32),
        jax.ShapeDtypeStruct((2, *block), f32),
    )
    operands = (stretch_slot, span_length, wet_mask, accum)
    sizes = (groups, chips, layers, pair_most, blocks_dev, all_blocks)

    def exchange(kernel, scratch, number):
        return pl.pallas_call(
            kernel,
            out_shape=shapes,
            in_specs=[smem, smem, smem, vmem],
            out_specs=(hbm, hbm),
            scratch_shapes=scratch,
            compiler_params=pltpu.CompilerParams(collective_id=number, has_side_effects=True),
        )

    def direct(*given):
        scratch = [pltpu.SMEM((devices,), jnp.int32), rows, rows, pair, pair]
        scratch += [sems((devices,))] * 3 + [sems((2,)), sems((2,)), sems]
        return exchange(functools.partial(exchange_kernel, sizes), scratch, 0)(*given)

    def stream(number, spare, early):
        def run(*given):
            rests = devices // layers
            main = rests * pair_most // 2
            room = main + spare

            def many(*count):
                return pltpu.VMEM((*count, *block), f32)

            scratch = [pltpu.SMEM((devices + 1,), jnp.int32), many(blocks_dev), many(room + 1)]
            scratch += [many(spare + 1), many(main), many(main), many(3, room + 1), many(3, room)]
            scratch += [many(4 * rests * pair_most), many(), many(rests)]
            scratch += [sems, sems, sems((2,)), sems, sems((2,)), sems, sems, sems((2, 3))]
            scratch += [sems, sems, sems, sems]
            return pl.pallas_call(
                functools.partial(stream_kernel, sizes, spare, early),
                out_shape=shapes,
                in_specs=[smem, smem, smem, hbm],
                out_specs=(vmem, vmem),
                scratch_shapes=scratch,
                compiler_params=pltpu.CompilerParams(collective_id=number, has_side_effects=True),
            )(*given)

        return run

    ready = devices & (devices - 1) == 0 and 4 * devices <= cells
    if layers == 4 and groups == 2 and pair_most >= 8 and ready:
        main = (devices // layers) * pair_most // 2
        spares = [(main * spare // 32, main * early // 32) for spare, early in SPARES]
        choice = pl.pallas_call(
            functools.partial(choose_kernel, (groups, chips, layers), main, spares),
            out_shape=jax.ShapeDtypeStruct((1,), jnp.int32),
            in_specs=[smem],
            out_specs=smem,
        )(span_length)[0]
        branches = [stream(number + 1, *spare) for number, spare in enumerate(spares)] + [direct]
        received, halo = lax.switch(choice, branches, *operands)
    else:
        received, halo = direct(*operands)
    return pl.pallas_call(
        functools.partial(filter_kernel, (groups, chips, pair_most, blocks_dev, all_blocks)),
        out_shape=shapes[0],
        in_specs=[smem, smem, smem, smem, vmem, vmem],
        out_specs=hbm,
        scratch_shapes=[pltpu.SMEM((devices + 1,), jnp.int32), rows, sems],
    )(stretch_slot, span_length, wet_mask, step_count, received, halo)


def solution(mesh):
    return jax.shard_map(
        on_device,
        mesh=mesh,
        in_specs=(P(("grp", "dev"), None, None), P(), P(), P(), P(("grp", "dev"))),
        out_specs=P(("grp", "dev"), None, None),
        check_vma=False,
    )
```

```python
import functools
import jax
import jax.numpy as jnp
from jax import lax
from jax.experimental import pallas as pl
from jax.experimental.pallas import tpu as pltpu
from jax.sharding import PartitionSpec as P

MESH = pl.DeviceIdType.MESH
SPARES = ((4, 24), (6, 24), (8, 24), (10, 24), (12, 24), (14, 24), (16, 24), (20, 24), (8, 28), (12, 28), (16, 28), (20, 28), (32, 32))


def exchange_kernel(
    sizes, stretch, spans, wet, accum, received, halo,
    starts, packed, landed, edge_out, edge_in, send_sem, recv_sem, out_sem, edge_send, edge_recv, edge_copy,
):
    groups, chips, layers, pair_most, blocks_dev, all_blocks = sizes
    devices = groups * chips
    plane = chips // layers
    grp = lax.axis_index("grp")
    dev = lax.axis_index("dev")
    me = grp * chips + dev
    layer, place = dev // plane, dev % plane

    def at(index):
        return (index // chips, index % chips)

    barrier = pltpu.get_barrier_semaphore()

    @pl.loop(1, devices)
    def _(step):
        pl.semaphore_signal(barrier, inc=1, device_id=at((me + step) % devices), device_id_type=MESH)

    def prefix(owner, total):
        starts[owner] = total
        return total + spans[owner]

    lax.fori_loop(0, devices, prefix, jnp.int32(0))

    def find(block, found):
        return jnp.where(stretch[block] // blocks_dev == me, block, found)

    phase = lax.fori_loop(0, devices, find, jnp.int32(0), unroll=8)

    def partner(turn, rest):
        there = ((layer + turn) % layers) * plane + (place + rest % plane) % plane
        return ((grp + rest // plane) % groups) * chips + there

    def pack(owner, target, base):
        start = starts[owner]
        first = start + lax.rem(phase - start + all_blocks * devices, devices)
        for rank in range(pair_most):
            block = jnp.minimum(first + rank * devices, all_blocks - 1)
            slot = lax.rem(stretch[block], blocks_dev)
            target[base + rank] = accum[slot]

    def send_copy(other):
        return pltpu.make_async_remote_copy(
            src_ref=packed.at[pl.ds(other * pair_most, pair_most)],
            dst_ref=landed.at[pl.ds(me * pair_most, pair_most)],
            send_sem=send_sem.at[other],
            recv_sem=recv_sem.at[me],
            device_id=at(other),
            device_id_type=MESH,
        )

    def out_copy(other):
        return pltpu.make_async_copy(
            landed.at[pl.ds(other * pair_most, pair_most)],
            received.at[pl.ds(other * pair_most, pair_most)],
            out_sem.at[other],
        )

    turns = [layers // 2] + [t for t in range(1, layers) if t != layers // 2]
    if layers > 1:
        turns = turns + [0]
    else:
        turns = [0]
    rests = groups * plane
    for number, turn in enumerate(turns):
        low = 1 if turn == 0 else 0

        @pl.loop(low, rests)
        def _(rest):
            other = partner(turn, rest)
            pack(other, packed, other * pair_most)

        if number == 0:
            pl.semaphore_wait(barrier, devices - 1)

        @pl.loop(low, rests)
        def _(rest):
            send_copy(partner(turn, rest)).start()

    pack(me, landed, me * pair_most)

    for turn in reversed(turns):
        low = 1 if turn == 0 else 0

        @pl.loop(low, rests)
        def _(rest):
            other = partner(turn, rest)
            pltpu.make_async_remote_copy(
                src_ref=packed.at[pl.ds(other * pair_most, pair_most)],
                dst_ref=landed.at[pl.ds(other * pair_most, pair_most)],
                send_sem=send_sem.at[other],
                recv_sem=recv_sem.at[other],
                device_id=at(other),
                device_id_type=MESH,
            ).wait_recv()
            out_copy(other).start()

    out_copy(me).start()

    start = starts[me]
    length = spans[me]
    first_from = stretch[start] // blocks_dev
    last = jnp.maximum(length - 1, 0)
    last_from = stretch[start + last] // blocks_dev
    edge_out[0] = landed[last_from * pair_most + last // devices] * (
        wet[last] == 1
    ).astype(jnp.float32)
    edge_out[1] = landed[first_from * pair_most] * (wet[0] == 1).astype(jnp.float32)
    copies = []
    for side, shift in ((0, 1), (1, devices - 1)):
        copies.append(
            pltpu.make_async_remote_copy(
                src_ref=edge_out.at[side],
                dst_ref=edge_in.at[side],
                send_sem=edge_send.at[side],
                recv_sem=edge_recv.at[side],
                device_id=at((me + shift) % devices),
                device_id_type=MESH,
            )
        )
    for copy in copies:
        copy.start()

    @pl.loop(1, devices)
    def _(step):
        send_copy((me + step) % devices).wait_send()

    @pl.loop(0, devices)
    def _(other):
        out_copy(other).wait()

    for copy in copies:
        copy.wait()
    final = pltpu.make_async_copy(edge_in, halo, edge_copy)
    final.start()
    final.wait()


def stream_kernel(
    sizes, spare, early, stretch, spans, wet, accum_at, received, halo,
    starts, accum, to_mate, to_spare, to_near, to_far, lists, merged, forward, edge_all, edge_near,
    load_sem, mate_send, mate_recv, spare_send, spare_recv, pass_send, main_send, main_recv,
    near_send, near_recv, edge_send, edge_recv,
):
    groups, chips, layers, pair_most, blocks_dev, all_blocks = sizes
    devices = groups * chips
    plane = chips // layers
    rests = groups * plane
    main = rests * pair_most // 2
    room = main + spare
    _, fields, cells = accum.shape
    shift = devices.bit_length() - 1
    grp = lax.axis_index("grp")
    dev = lax.axis_index("dev")
    me = grp * chips + dev
    layer, place = dev // plane, dev % plane
    low = layer < 2
    inner = (layer == 1) | (layer == 2)
    across = (
        layer, layer + 1 - 2 * (layer % 2), jnp.where(low, 2, 1), jnp.where(low, 3, 0)
    )
    my_spot = grp * plane + place

    def at(index):
        return (index // chips, index % chips)

    def column(there):
        return grp * chips + there * plane + place

    def mate(spot):
        return (spot // plane) * chips + layer * plane + spot % plane

    load = pltpu.make_async_copy(accum_at, accum, load_sem)
    load.start()
    barrier = pltpu.get_barrier_semaphore()
    for turn in (1, 2, 3):
        pl.semaphore_signal(
            barrier, inc=1, device_id=at(column((layer + turn) % layers)), device_id_type=MESH
        )

    @pl.loop(1, rests)
    def _(step):
        pl.semaphore_signal(
            barrier, inc=1, device_id=at(mate((my_spot + step) % rests)), device_id_type=MESH
        )

    def prefix(owner, total):
        starts[owner] = total
        return total + spans[owner]

    starts[devices] = lax.fori_loop(0, devices, prefix, jnp.int32(0), unroll=8)

    def find(block, found):
        holder = lax.div(stretch[block], blocks_dev)
        return tuple(
            jnp.where(holder == column(across[turn]), block, found[turn]) for turn in range(4)
        )

    phases = lax.fori_loop(0, devices, find, (jnp.int32(0),) * 4, unroll=8)

    def rank_of(phase, owner):
        return lax.shift_right_arithmetic(starts[owner] + (devices - 1) - phase, jnp.int32(shift))

    def layer_list(phase, there):
        marks = []
        for part in range(2):
            first = part * chips + there * plane
            begin = rank_of(phase, first)
            marks.append((begin, rank_of(phase, first + plane) - begin))
        (begin_low, amount), (begin_high, more) = marks
        return amount, begin_low, begin_high - amount, amount + more

    def slot_of(rank, phase):
        block = jnp.minimum(phase + rank * devices, all_blocks - 1)
        return lax.rem(stretch[block], blocks_dev)

    mine = phases[0]
    lists_to = [layer_list(mine, across[turn]) for turn in range(4)]

    def block_at(listed, spot):
        amount, begin_low, begin_high, _ = listed
        return accum[slot_of(spot + jnp.where(spot < amount, begin_low, begin_high), mine)]

    def fill(target, begin, end, listed):
        def one(spot, carry):
            target[spot] = block_at(listed, spot)
            return carry

        lax.fori_loop(begin, end, one, jnp.int32(0), unroll=4)

    far_list = jnp.where(inner, 1, 2)

    def pick(turn, values):
        if turn == "first":
            return jnp.where(inner, values[2], values[3])
        if turn == "second":
            return jnp.where(inner, values[3], values[2])
        return values[turn]

    def order(turn):
        return {"first": 2, "second": 3}.get(turn, turn)

    def mate_copy(step):
        begin, end = ((0, early), (early, room + 1))[step]
        return pltpu.make_async_remote_copy(
            src_ref=to_mate.at[pl.ds(begin, end - begin)],
            dst_ref=lists.at[0, pl.ds(begin, end - begin)],
            send_sem=mate_send,
            recv_sem=mate_recv.at[step],
            device_id=at(column(across[1])),
            device_id_type=MESH,
        )

    def spare_copy(where):
        return pltpu.make_async_remote_copy(
            src_ref=to_spare,
            dst_ref=lists.at[where, pl.ds(main, spare + 1)],
            send_sem=spare_send,
            recv_sem=spare_recv.at[where - 1],
            device_id=at(column(across[2])),
            device_id_type=MESH,
        )

    def pass_copy(where):
        return pltpu.make_async_remote_copy(
            src_ref=lists.at[where, pl.ds(main, spare + 1)],
            dst_ref=lists.at[where, pl.ds(main, spare + 1)],
            send_sem=pass_send,
            recv_sem=spare_recv.at[where - 1],
            device_id=at(column(across[1])),
            device_id_type=MESH,
        )

    third = main // 2
    cuts = [(0, third), (third, early), (early, main)] if early < main else [(0, third), (third, main)]
    last = len(cuts) - 1
    stops = [plane // 2, plane, rests] if early < main else [plane // 2, rests]
    groups_of = list(zip([0] + stops[:-1], stops, [end for _, end in cuts[:-1]] + [room]))

    def main_copy(outer, step, where):
        begin, end = cuts[step]
        return pltpu.make_async_remote_copy(
            src_ref=(to_far if outer else to_near).at[pl.ds(begin, end - begin)],
            dst_ref=lists.at[where, pl.ds(begin, end - begin)],
            send_sem=main_send,
            recv_sem=main_recv.at[where - 1, step],
            device_id=at(column(across[3 if outer else 2])),
            device_id_type=MESH,
        )

    def near_copy(turn, spot, sender):
        return pltpu.make_async_remote_copy(
            src_ref=forward.at[pl.ds((order(turn) * rests + spot) * pair_most, pair_most)],
            dst_ref=received.at[pl.ds(sender * pair_most, pair_most)],
            send_sem=near_send,
            recv_sem=near_recv,
            device_id=at(mate(spot)),
            device_id_type=MESH,
        )

    def edge_copy(spot, sender):
        return pltpu.make_async_remote_copy(
            src_ref=edge_all,
            dst_ref=edge_near.at[sender],
            send_sem=edge_send,
            recv_sem=edge_recv,
            device_id=at(mate(spot)),
            device_id_type=MESH,
        )

    def whole(held, count, send_sem, recv_sem):
        part = held.at[pl.ds(0, count)]
        return pltpu.make_async_remote_copy(
            src_ref=part,
            dst_ref=part,
            send_sem=send_sem,
            recv_sem=recv_sem,
            device_id=at(column(across[1])),
            device_id_type=MESH,
        )

    def hand_on(turn, begin, end, limit):
        listed = pick(turn, (0, 0, 1, 2))
        phase = pick(turn, phases)
        sender = column(pick(turn, across))
        if turn != 0:
            amount, begin_low, begin_high, _ = layer_list(phase, layer)
            jump = jnp.int32(0)
            if turn != 1:
                other = layer_list(phase, across[1])[3]
                jump = jnp.where(inner, jnp.maximum(other - main, 0), 0)

        def put(spot, target, base):
            owner = mate(spot)
            first = rank_of(phase, owner)
            if turn != 0:
                first = first - jnp.where(spot < plane, begin_low, begin_high)
            for step in range(pair_most):
                if turn == 0:
                    target[base + step] = accum[slot_of(first + step, phase)]
                else:
                    row = first + step
                    if turn != 1:
                        row = row + jnp.where(row < main, 0, jump)
                    target[base + step] = merged[listed, jnp.clip(row, 0, limit - 1)]

        @pl.loop(begin, end)
        def _(spot):
            @pl.when(spot != my_spot)
            def _():
                put(spot, forward, (order(turn) * rests + spot) * pair_most)

            @pl.when(spot == my_spot)
            def _():
                put(spot, received, sender * pair_most)

        @pl.loop(begin, end)
        def _(spot):
            @pl.when(spot != my_spot)
            def _():
                near_copy(turn, spot, sender).start()

    load.wait()
    fill(to_mate, 0, early, lists_to[1])

    @pl.when(inner)
    def _():
        fill(to_far, 0, cuts[last][0], lists_to[3])

    pl.semaphore_wait(barrier, layers - 1 + rests - 1)
    mate_copy(0).start()

    @pl.when(inner)
    def _():
        for step in range(last):
            main_copy(1, step, far_list).start()

    hand_on(0, 0, rests, None)

    lane = lax.broadcasted_iota(jnp.int32, (fields, cells), 1)
    ending = jnp.maximum(spans[me] - 1, 0)
    edges = jnp.where(
        lane == 2 * (devices + me),
        jnp.where(wet[0] == 1, 1.0, 0.0),
        jnp.where(
            lane == 2 * (devices + me) + 1, jnp.where(wet[ending] == 1, 1.0, 0.0), 0.0
        ),
    )

    def collect(owner, edges):
        for back, turned in ((1, 2 * owner), (0, 2 * owner - 1)):
            held = stretch[jnp.clip(starts[owner] - back, 0, all_blocks - 1)]
            rolled = pltpu.roll(accum[lax.rem(held, blocks_dev)], (turned + back) % cells, 1)
            wanted = jnp.where(lax.div(held, blocks_dev) == me, turned, -1)
            edges = jnp.where(lane == wanted, rolled, edges)
        return edges

    edges = lax.fori_loop(1, devices, collect, edges, unroll=2)
    to_mate[room] = edges
    to_spare[spare] = edges
    over = jnp.maximum(lists_to[3][3] - main, 0)

    def fill_spare(spot, carry):
        rank = []
        for listed, back in ((lists_to[3], 0), (lists_to[2], over)):
            amount, begin_low, begin_high, _ = listed
            there = main + spot - back
            rank.append(there + jnp.where(there < amount, begin_low, begin_high))
        to_spare[spot] = accum[slot_of(jnp.where(spot < over, rank[0], rank[1]), mine)]
        return carry

    lax.fori_loop(0, spare, fill_spare, jnp.int32(0), unroll=2)
    fill(to_mate, early, room, lists_to[1])
    spare_copy(far_list).start()
    mate_copy(1).start()
    last = len(cuts) - 1

    @pl.when(inner)
    def _():
        fill(to_near, 0, main, lists_to[2])
        for step in range(last):
            main_copy(0, step, far_list).start()
        fill(to_far, *cuts[last], lists_to[3])
        main_copy(1, last, far_list).start()
        main_copy(0, last, far_list).start()

    @pl.when(jnp.logical_not(inner))
    def _():
        for step in range(last + 1):
            fill(to_near, *cuts[step], lists_to[2])
            fill(to_far, *cuts[step], lists_to[3])
            main_copy(0, step, far_list).start()
            main_copy(1, step, far_list).start()

    def merge(where, begin, end):
        part = pl.ds(begin, end - begin)
        merged[where, part] = lists[where, part]

    def arrive(where, step):
        main_copy(0, step, where).wait_recv()
        merge(where, *cuts[step])

    def spared(where):
        spare_copy(where).wait_recv()
        merge(where, main, room)

    def advance(where, step):
        arrive(where, step)
        hand_on(where + 1, *groups_of[step])

    def sum_edges():
        total = edges
        for where in range(3):
            total = total + lists[where, room]
        edge_all[...] = total

        @pl.loop(0, rests)
        def _(spot):
            @pl.when(spot != my_spot)
            def _():
                edge_copy(spot, my_spot).start()

    mate_copy(0).wait_recv()
    merge(0, 0, early)
    hand_on(1, 0, plane, early)

    @pl.when(inner)
    def _():
        spared(1)
        pass_copy(1).start()
        spared(2)
        pass_copy(2).start()

    @pl.when(jnp.logical_not(inner))
    def _():
        for step in range(last):
            advance(1, step)

    mate_copy(1).wait_recv()
    merge(0, early, room)
    hand_on(1, plane, rests, room)

    @pl.when(inner)
    def _():
        sum_edges()

    for step in range(last):
        advance(2, step)

    @pl.when(jnp.logical_not(inner))
    def _():
        spared(2)
        spared(1)
        sum_edges()

    advance(2, last)

    @pl.when(inner)
    def _():
        for step in range(last):
            advance(1, step)

    advance(1, last)

    @pl.when(inner)
    def _():
        whole(forward, 2 * (spare + 1), pass_send, near_recv).wait_send()

    whole(forward, room + 1, mate_send, near_recv).wait_send()
    spare_copy(far_list).wait_send()
    whole(forward, 2 * main, main_send, near_recv).wait_send()

    edge_near[my_spot] = edge_all[...]

    whole(edge_near, rests - 1, edge_send, edge_recv).wait()
    total = edge_near[0]
    for spot in range(1, rests):
        total = total + edge_near[spot]
    spread = cells * devices

    def cell(to, lane_from):
        return pltpu.roll(total, lax.rem(to - lane_from + spread, cells), 1)

    wet_left, wet_right = 2 * (devices + me) - 1, 2 * (devices + me) + 2
    halo[0] = cell(cells - 1, 2 * me) * cell(cells - 1, wet_left)
    halo[1] = cell(0, 2 * me + 1) * cell(0, wet_right)

    near_all = 4 * (rests - 1) * pair_most
    whole(forward, near_all, near_send, near_recv).wait_send()
    whole(received, near_all, near_send, near_recv).wait_recv()


def filter_kernel(sizes, stretch, spans, wet, counts, received, halo, out, rows, done, sem):
    groups, chips, pair_most, blocks_dev, all_blocks = sizes
    devices = groups * chips
    me = lax.axis_index("grp") * chips + lax.axis_index("dev")
    length = spans[me]
    capacity = wet.shape[0]
    _, fields, cells = halo.shape
    start = lax.fori_loop(
        0, devices, lambda o, s: s + jnp.where(o < me, spans[o], 0), jnp.int32(0), unroll=8
    )

    def fill(spot, carry):
        block = jnp.minimum(start + spot, all_blocks - 1)
        rows[spot] = lax.div(stretch[block], blocks_dev) * pair_most
        return carry

    lax.fori_loop(0, devices, fill, jnp.int32(0), unroll=8)
    rows[devices] = rows[0] + 1
    field = lax.broadcasted_iota(jnp.int32, (fields, cells), 0)
    held = jnp.ones((fields, cells), jnp.int32)
    for index in range(fields):
        held = jnp.where(field == index, counts[index], held)
    scale = 0.25 / held.astype(jnp.float32)
    lane = lax.broadcasted_iota(jnp.int32, (fields, cells), 1)
    at_first, at_last = lane == 0, lane == cells - 1
    left = halo[0] * jnp.where(me > 0, 1.0, 0.0)
    right = halo[1] * jnp.where(me < devices - 1, 1.0, 0.0)

    def wet_of(slot):
        return jnp.where(slot < length, wet[slot], 0).astype(jnp.float32)

    def out_copy(rank):
        part = pl.ds(rank * devices, devices)
        return pltpu.make_async_copy(done.at[part], out.at[part], sem)

    def one_rank(rank, carry):
        def one(spot, carry):
            before, here, mask = carry
            slot = rank * devices + spot
            later = jnp.minimum(slot + 1, capacity - 1)
            later_mask = wet_of(later)
            row = jnp.minimum(rows[spot + 1] + rank, capacity - 1)
            after = jnp.where(slot + 1 == length, right, received[row] * later_mask)
            low = pltpu.roll(jnp.where(at_last, before, here), 1, 1)
            high = pltpu.roll(jnp.where(at_first, after, here), cells - 1, 1)
            done[slot] = (low + high + 2.0 * here) * (scale * mask)
            return here, after, later_mask

        carry = lax.fori_loop(0, devices, one, carry, unroll=min(devices, 32))
        out_copy(rank).start()
        return carry

    mask = wet_of(jnp.int32(0))
    lax.fori_loop(0, pair_most, one_rank, (left, received[rows[0]] * mask, mask))

    pltpu.make_async_copy(done, out, sem).wait()


def choose_kernel(sizes, main, spares, spans, out):
    groups, chips, layers = sizes
    devices = groups * chips
    plane = chips // layers
    over, most = [], jnp.int32(0)
    for layer in range(layers):
        need = jnp.int32(0)
        for grp in range(groups):
            part = jnp.int32(0)
            for spot in range(plane):
                part = part + spans[grp * chips + layer * plane + spot]
            part = lax.div(part + devices - 1, devices)
            if grp == 0:
                most = jnp.maximum(most, part)
            need = need + part
        over.append(jnp.maximum(need - main, 0))
    need = jnp.maximum(over[0] + over[1], over[2] + over[3])
    choice = jnp.int32(len(spares))
    for number, (spare, early) in reversed(list(enumerate(spares))):
        choice = jnp.where((need <= spare) & (most <= early), number, choice)
    out[0] = choice


def on_device(accum, step_count, stretch_slot, span_length, wet_mask):
    groups, chips = lax.axis_size("grp"), lax.axis_size("dev")
    devices = groups * chips
    blocks_dev, fields, cells = accum.shape
    capacity = wet_mask.shape[0]
    pair_most = capacity // devices
    all_blocks = stretch_slot.shape[0]
    layers = 4 if chips % 4 == 0 else 1
    smem = pl.BlockSpec(memory_space=pltpu.SMEM)
    vmem = pl.BlockSpec(memory_space=pltpu.VMEM)
    hbm = pl.BlockSpec(memory_space=pl.ANY)
    block = (fields, cells)
    f32 = jnp.float32
    sems = pltpu.SemaphoreType.DMA
    rows = pltpu.VMEM((capacity, *block), f32)
    pair = pltpu.VMEM((2, *block), f32)
    shapes = (
        jax.ShapeDtypeStruct((capacity, *block), f32),
        jax.ShapeDtypeStruct((2, *block), f32),
    )
    operands = (stretch_slot, span_length, wet_mask, accum)
    sizes = (groups, chips, layers, pair_most, blocks_dev, all_blocks)

    def exchange(kernel, scratch, number):
        return pl.pallas_call(
            kernel,
            out_shape=shapes,
            in_specs=[smem, smem, smem, vmem],
            out_specs=(hbm, hbm),
            scratch_shapes=scratch,
            compiler_params=pltpu.CompilerParams(collective_id=number, has_side_effects=True),
        )

    def direct(*given):
        scratch = [pltpu.SMEM((devices,), jnp.int32), rows, rows, pair, pair]
        scratch += [sems((devices,))] * 3 + [sems((2,)), sems((2,)), sems]
        return exchange(functools.partial(exchange_kernel, sizes), scratch, 0)(*given)

    def stream(number, spare, early):
        def run(*given):
            rests = devices // layers
            main = rests * pair_most // 2
            room = main + spare

            def many(*count):
                return pltpu.VMEM((*count, *block), f32)

            scratch = [pltpu.SMEM((devices + 1,), jnp.int32), many(blocks_dev), many(room + 1)]
            scratch += [many(spare + 1), many(main), many(main), many(3, room + 1), many(3, room)]
            scratch += [many(4 * rests * pair_most), many(), many(rests)]
            scratch += [sems, sems, sems((2,)), sems, sems((2,)), sems, sems, sems((2, 3))]
            scratch += [sems, sems, sems, sems]
            return pl.pallas_call(
                functools.partial(stream_kernel, sizes, spare, early),
                out_shape=shapes,
                in_specs=[smem, smem, smem, hbm],
                out_specs=(vmem, vmem),
                scratch_shapes=scratch,
                compiler_params=pltpu.CompilerParams(collective_id=number, has_side_effects=True),
            )(*given)

        return run

    ready = devices & (devices - 1) == 0 and 4 * devices <= cells
    if layers == 4 and groups == 2 and pair_most >= 8 and ready:
        main = (devices // layers) * pair_most // 2
        spares = [(main * spare // 32, main * early // 32) for spare, early in SPARES]
        choice = pl.pallas_call(
            functools.partial(choose_kernel, (groups, chips, layers), main, spares),
            out_shape=jax.ShapeDtypeStruct((1,), jnp.int32),
            in_specs=[smem],
            out_specs=smem,
        )(span_length)[0]
        branches = [stream(number + 1, *spare) for number, spare in enumerate(spares)] + [direct]
        received, halo = lax.switch(choice, branches, *operands)
    else:
        received, halo = direct(*operands)
    return pl.pallas_call(
        functools.partial(filter_kernel, (groups, chips, pair_most, blocks_dev, all_blocks)),
        out_shape=shapes[0],
        in_specs=[smem, smem, smem, smem, vmem, vmem],
        out_specs=hbm,
        scratch_shapes=[pltpu.SMEM((devices + 1,), jnp.int32), rows, sems],
    )(stretch_slot, span_length, wet_mask, step_count, received, halo)


def solution(mesh):
    return jax.shard_map(
        on_device,
        mesh=mesh,
        in_specs=(P(("grp", "dev"), None, None), P(), P(), P(), P(("grp", "dev"))),
        out_specs=P(("grp", "dev"), None, None),
        check_vma=False,
    )
```
